128 devices in a mesh: pts: 16 (over z_hi, x, core), wlk: 8 (over z_lo, y).
Axes of the slice: x: 4, y: 4, z: 4 (z_hi: 2, z_lo: 2; z = z_hi * 2 + z_lo), core: 2. Of those that a mesh axis runs over, the one named last changes fastest.
Arguments:
- green_half: bfloat16 [16, 400, 2400], P('wlk'), may hold values from -6 to 6
- collocation: bfloat16 [2400, 9600], P('wlk', 'pts'), may hold values from -0.125 to 0.125
- occupied: bfloat16 [9600, 400], P('pts'), may hold values from -0.0029296875 to 0.0029296875
- kernel: bfloat16 [9600, 9600], P('pts'), may hold values from 0 to 16, as said below
Outputs:
- potential: float32 [16, 9600], P('wlk', 'pts')
- coulomb_energy: float32 [16], P('wlk')
- exchange_energy: float32 [16], P('wlk')
The draws below stay inside these ranges and needn't reach their ends.
Inputs may be any that keep to these rules, and one draw needn't show every extreme that they name: kernel is symmetric and positive definite: kernel[p, q] equals kernel[q, p].
All inputs are finite; a program needn't handle non-finite values.
Results may differ from the reference program's by a relative error of at most 0.008.
Values may be sent and summed in bfloat16 or wider, within the bound.
No kernel may reach another device: no remote copies, remote signals or barrier semaphores. Data moves between devices by JAX's collectives and lax.ppermute only.
A program may use at most 192 MiB of HBM per device.

```python
import jax
import jax.numpy as jnp
from jax import lax

ORB = 2400
ELEC = 400
RANK = 9600
W = 16


def draw_kernel(key, part):
    point_spots = jax.random.uniform(jax.random.fold_in(key, 3), (RANK, 3), jnp.float32, 0.0, 1.0)
    length = (10.0 / RANK) ** (1.0 / 3.0)
    squared = jnp.zeros((RANK, RANK), jnp.float32)
    for column in range(3):
        offset = point_spots[:, column][:, None] - point_spots[:, column][None, :]
        squared = squared + offset * offset
    distance = jnp.sqrt(squared)
    values = 6.0 * jnp.exp(-distance / length) + 1.5 * jnp.eye(RANK, dtype=jnp.float32)
    return values.astype(jnp.bfloat16)


def block_scale(own_key, extent, split, smallest, largest):
    level, own = 1.0, jax.random.fold_in(own_key, 6)
    for axis_at, shards_of in split:
        draws = jnp.exp(jax.random.uniform(jax.random.fold_in(own, axis_at), (shards_of,), jnp.float32, smallest / len(split), largest / len(split)))
        level = level * jnp.repeat(draws, extent[axis_at] // shards_of).reshape([-1 if axis == axis_at else 1 for axis in range(len(extent))])
    return level


def noise(rng, shape, scale, limit, split=(), held_as=jnp.bfloat16):
    values = scale * jax.random.normal(rng, shape, jnp.float32)
    if split:
        values = values * block_scale(rng, shape, split, -0.22, 0.18)
    return jnp.clip(values, -limit, limit).astype(held_as)


def setup_inputs(seed: int = 0) -> dict:
    arg_keys = jax.random.split(jax.random.key(seed), 5)
    return {
        "green_half": noise(arg_keys[0], (W, ELEC, ORB), 1.0, 6.0, ((0, 8),)),
        "collocation": noise(arg_keys[1], (ORB, RANK), ORB ** -0.5, 0.125, ((0, 8), (1, 16))),
        "occupied": noise(arg_keys[2], (RANK, ELEC), (RANK * ELEC) ** -0.5, 0.0029296875, ((0, 16),)),
        "kernel": draw_kernel(jax.random.fold_in(arg_keys[4], 71), 0),
    }


def reference(green_half, collocation, occupied, kernel):
    kernel_float = kernel.astype(jnp.float32)

    def one_walker(green_one):
        theta = jnp.dot(green_one, collocation, preferred_element_type=jnp.float32).astype(jnp.bfloat16)
        density = jnp.sum(theta.astype(jnp.float32) * occupied.T.astype(jnp.float32), axis=0)
        density_b = density.astype(jnp.bfloat16)
        potential = jnp.dot(kernel, density_b, preferred_element_type=jnp.float32)
        coulomb = 0.5 * jnp.sum(density * potential)
        cross = jnp.dot(theta.T, occupied.T, preferred_element_type=jnp.float32)
        exchange = -0.5 * jnp.sum(kernel_float * cross * cross.T)
        return potential, coulomb, exchange

    potential, coulomb, exchange = lax.map(one_walker, green_half)
    return potential, coulomb, exchange
```

```python
import jax
import jax.numpy as jnp
from jax import lax
from jax.experimental import pallas as pl
from jax.experimental.pallas import tpu as pltpu
from jax.sharding import PartitionSpec as P


F32 = jnp.float32
BF16 = jnp.bfloat16
PLANES, COLS, CORES = 2, 4, 2
ZLO, YS = 2, 4
EXTRA = 8


def whole():
    return pl.BlockSpec(memory_space=pltpu.VMEM)


def pts_id(a, x, c):
    return ((a % PLANES) * COLS + x % COLS) * CORES + c % CORES


def from_chip(block, da, dx, dc=0):
    route = [
        (pts_id(a + da, x + dx, c + dc), pts_id(a, x, c))
        for a in range(PLANES)
        for x in range(COLS)
        for c in range(CORES)
    ]
    return lax.ppermute(block, "pts", route)


def from_group(block, dz, dy):
    route = [
        ((z + dz) % ZLO * YS + (y + dy) % YS, z * YS + y) for z in range(ZLO) for y in range(YS)
    ]
    return lax.ppermute(block, "wlk", route)


def split_columns(array, pieces, steps):
    rows, cols = array.shape
    width = cols // pieces
    tile = rows // steps

    def body(x_ref, o_ref):
        for b in range(pieces):
            o_ref[b] = x_ref[:, b * width : (b + 1) * width]

    return pl.pallas_call(
        body,
        grid=(steps,),
        in_specs=[pl.BlockSpec((tile, cols), lambda i: (i, 0))],
        out_specs=pl.BlockSpec((pieces, tile, width), lambda i: (0, i, 0)),
        out_shape=jax.ShapeDtypeStruct((pieces, rows, width), array.dtype),
        name="split_columns",
    )(array)


def theta_part(green_cut, blocks, order, rest=None):
    n = len(blocks)
    rows = green_cut.shape[1]
    pts = blocks[0].shape[1]

    def g_spec(j):
        return pl.BlockSpec((1, rows, green_cut.shape[2]), lambda i, s: (s[j], 0, 0))

    g_specs = [g_spec(j) for j in range(n)]
    flops = 2 * rows * pts * green_cut.shape[2] * n
    cost = pl.CostEstimate(flops=flops, bytes_accessed=flops // 600, transcendentals=0)

    if rest is None:

        def first(s_ref, *refs):
            gs, cs, o_ref = refs[:n], refs[n : 2 * n], refs[2 * n]
            o_ref[...] = sum(
                jnp.dot(gs[j][0], cs[j][...], preferred_element_type=F32) for j in range(n)
            )

        return pl.pallas_call(
            first,
            grid_spec=pltpu.PrefetchScalarGridSpec(
                num_scalar_prefetch=1,
                grid=(1,),
                in_specs=g_specs + [whole()] * n,
                out_specs=whole(),
            ),
            out_shape=jax.ShapeDtypeStruct((rows, pts), F32),
            cost_estimate=cost,
            name="theta_first",
        )(order, *[green_cut] * n, *blocks)

    so_far, occ_t = rest
    elec = occ_t.shape[0]

    def last(s_ref, *refs):
        gs, cs = refs[:n], refs[n : 2 * n]
        acc_ref, occ_ref, t0_ref, t1_ref, ta_ref, tb_ref, tc_ref, ts_ref, dens_ref = refs[2 * n :]
        th_refs = (t0_ref, t1_ref)
        occ = occ_ref[...].astype(F32)
        dens = []
        for w in range(2):
            at = pl.ds(w * elec, elec)
            t = acc_ref[at, :] + sum(
                jnp.dot(gs[j][0, at, :], cs[j][...], preferred_element_type=F32) for j in range(n)
            )
            t = t.astype(BF16)
            th_refs[w][0:elec, :] = t
            dens.append(jnp.sum(t.astype(F32) * occ, axis=0, keepdims=True))
        dens_ref[0:1, :] = dens[0]
        dens_ref[1:2, :] = dens[1]
        row = lax.broadcasted_iota(jnp.int32, (EXTRA, pts), 0)
        tail = jnp.where(row == 0, dens[0], jnp.where(row == 1, dens[1], 0.0)).astype(BF16)
        for w in range(2):
            th_refs[w][elec : elec + EXTRA, :] = tail
        for k, o_ref in enumerate((ta_ref, tb_ref, tc_ref, ts_ref)):
            w = s_ref[n + k]

            @pl.when(w == 0)
            def _():
                o_ref[...] = t0_ref[...]

            @pl.when(w != 0)
            def _():
                o_ref[...] = t1_ref[...]

    slab = jax.ShapeDtypeStruct((elec + EXTRA, pts), BF16)
    return pl.pallas_call(
        last,
        grid_spec=pltpu.PrefetchScalarGridSpec(
            num_scalar_prefetch=1,
            grid=(1,),
            in_specs=g_specs + [whole()] * (n + 2),
            out_specs=[whole()] * 7,
        ),
        out_shape=[slab] * 6 + [jax.ShapeDtypeStruct((2, pts), F32)],
        cost_estimate=cost,
        name="theta_last",
    )(order, *[green_cut] * n, *blocks, so_far, occ_t)


def exchange(jobs, where, theta_own, occ_own, kernel_cut, acc):
    n = len(jobs)
    pts, elec = occ_own.shape
    blk = kernel_cut.shape[2]

    def k_spec(j):
        return pl.BlockSpec((1, pts, blk), lambda i, s: (s[2 * j], 0, 0))

    def body(s_ref, *refs):
        ks, os, ts = refs[:n], refs[n : 2 * n], refs[2 * n : 3 * n]
        refs = refs[3 * n :]
        to_ref, oo_ref = refs[:2]
        if acc is None:
            ex_ref, pot_ref = refs[2:]
            ex_ref[...] = jnp.zeros_like(ex_ref)
            pot_ref[...] = jnp.zeros_like(pot_ref)
        else:
            ex_in, pot_in, ex_ref, pot_ref = refs[2:]
            ex_ref[...] = ex_in[...]
            pot_ref[...] = pot_in[...]
        for j, (_, _, weight, adds) in enumerate(jobs):
            w = s_ref[2 * j + 1]
            k = ks[j][0].astype(F32)
            near = jnp.dot(to_ref[w], os[j][...], preferred_element_type=F32)
            far = jnp.dot(oo_ref[...], ts[j][0:elec, :], preferred_element_type=F32)
            prod = k * near * far
            ex_ref[w] += weight * jnp.sum(prod.reshape(pts // 8, 8, blk), axis=0)
            if adds:
                dens = ts[j][elec : elec + EXTRA, :].astype(F32)
                lane = lax.broadcasted_iota(jnp.int32, (pts, 128), 1)
                p0 = jnp.sum(k * dens[0:1, :], axis=1, keepdims=True)
                p1 = jnp.sum(k * dens[1:2, :], axis=1, keepdims=True)
                pot_ref[...] += jnp.where(lane == 0, p0, jnp.where(lane == 1, p1, 0.0))

    shapes = [jax.ShapeDtypeStruct((2, 8, blk), F32), jax.ShapeDtypeStruct((pts, 128), F32)]
    flops = 4 * pts * blk * elec * n
    extra = () if acc is None else tuple(acc)
    return pl.pallas_call(
        body,
        grid_spec=pltpu.PrefetchScalarGridSpec(
            num_scalar_prefetch=1,
            grid=(1,),
            in_specs=[k_spec(j) for j in range(n)] + [whole()] * (2 * n + 2 + len(extra)),
            out_specs=[whole()] * 2,
        ),
        out_shape=shapes,
        cost_estimate=pl.CostEstimate(
            flops=flops, bytes_accessed=flops // 300, transcendentals=0
        ),
        name="exchange",
    )(
        where,
        *[kernel_cut] * n,
        *[job[0] for job in jobs],
        *[job[1] for job in jobs],
        theta_own,
        occ_own,
        *extra,
    )


def everyone_total(v):
    n = PLANES * COLS * CORES
    for bit in (1, 2, 4, 8):
        v = v + lax.ppermute(v, "pts", [(i, i ^ bit) for i in range(n)])
    return v


def local(green_half, collocation, occupied, kernel):
    walkers, elec, orb = green_half.shape
    orb_cut, pts = collocation.shape
    groups = ZLO * YS
    blocks = PLANES * COLS * CORES
    here = lax.axis_index("pts")
    plane, col, core = here // (COLS * CORES), here // CORES % COLS, here % CORES
    group = lax.axis_index("wlk")
    zlo, y = group // YS, group % YS
    occ_t = occupied.T

    coll = {(0, 0): collocation}
    coll[1, 0] = from_group(collocation, 1, 0)
    for dy in (1, 3, 2):
        coll[0, dy] = from_group(collocation, 0, dy)
    occ = {(0, 0): occ_t}
    occ[1, 0] = from_chip(occ_t, 1, 0)
    for dx in (1, 3, 2):
        occ[0, dx] = from_chip(occ_t, 0, dx)
    for dy in (1, 3, 2):
        coll[1, dy] = from_group(coll[1, 0], 0, dy)
    for dx in (1, 3, 2):
        occ[1, dx] = from_chip(occ[1, 0], 0, dx)

    green_cut = split_columns(green_half.reshape(walkers * elec, orb), groups, 4)
    kernel_cut = split_columns(kernel, blocks, 5)

    def order(keys, more=()):
        return jnp.stack(
            [(zlo + dz) % ZLO * YS + (y + dy) % YS for dz, dy in keys] + list(more)
        ).astype(jnp.int32)

    early = [(0, 0), (1, 0), (0, 1), (0, 3)]
    late = [(0, 2), (1, 1), (1, 3), (1, 2)]
    so_far = theta_part(green_cut, [coll[k] for k in early], order(early))
    low = (col < COLS // 2).astype(jnp.int32)
    takes = {(0, 3): 0 * low, (1, 3): 0 * low, (0, 1): 0 * low + 1, (1, 1): 0 * low + 1}
    takes[0, 2] = 1 - low
    takes[1, 2] = low
    takes[1, 0] = plane
    t0, t1, ta, tb, tc, ts, density = theta_part(
        green_cut,
        [coll[k] for k in late],
        order(late, (low, 1 - low, 1 - plane, 1 - core)),
        rest=(so_far, occ_t),
    )
    sends = {(0, 3): t0, (1, 3): t0, (0, 1): t1, (1, 1): t1, (0, 2): ta, (1, 2): tb, (1, 0): tc}
    hops = [(0, 3), (0, 1), (1, 0), (1, 3), (1, 1), (0, 2), (1, 2)]
    theta = {d: from_chip(sends[d], *d) for d in hops}
    theta_sib = {(0, 0): from_chip(ts, 0, 0, 1)}
    occ_sib = {d: from_chip(occ[d], 0, 0, 1) for d in [(0, 0)] + hops}

    theta_own = jnp.stack([t0[:elec].T, t1[:elec].T])

    def where(*entries):
        return jnp.stack([v for entry in entries for v in entry]).astype(jnp.int32)

    acc = exchange(
        [(occ_t, t0, 1.0, True), (occ_t, t1, 1.0, False)],
        where((here, 0 * here), (here, 0 * here + 1)),
        theta_own,
        occupied,
        kernel_cut,
        None,
    )
    other = pts_id(plane, col, core + 1)
    acc = exchange(
        [(occ_sib[0, 0], theta_sib[0, 0], 2.0, True)],
        where((other, core)),
        theta_own,
        occupied,
        kernel_cut,
        acc,
    )
    for d in hops:
        theta_sib[d] = from_chip(theta[d], 0, 0, 1)
        acc = exchange(
            [(occ[d], theta[d], 2.0, True), (occ_sib[d], theta_sib[d], 2.0, True)],
            where(
                (pts_id(plane + d[0], col + d[1], core), takes[d]),
                (pts_id(plane + d[0], col + d[1], core + 1), takes[d]),
            ),
            theta_own,
            occupied,
            kernel_cut,
            acc,
        )
    ex, pot = acc
    potential = pot[:, :walkers].T
    coulomb = 0.5 * jnp.sum(density * potential, axis=1)
    energies = everyone_total(jnp.concatenate([coulomb, -0.5 * jnp.sum(ex, axis=(1, 2))]))
    return potential, energies[:walkers], energies[walkers:]


def solution(mesh):
    placed = (P("wlk", None, None), P("wlk", "pts"), P("pts", None), P("pts", None))
    return jax.shard_map(
        local,
        mesh=mesh,
        in_specs=placed,
        out_specs=(P("wlk", "pts"), P("wlk"), P("wlk")),
        check_vma=False,
    )
```

```python
import jax
import jax.numpy as jnp
from jax import lax
from jax.experimental import pallas as pl
from jax.experimental.pallas import tpu as pltpu
from jax.sharding import PartitionSpec as P


F32 = jnp.float32
BF16 = jnp.bfloat16
PLANES, COLS, CORES = 2, 4, 2
ZLO, YS = 2, 4
EXTRA = 8
HOPS = [(0, 3), (0, 1), (1, 0), (1, 3), (1, 1), (0, 2), (1, 2)]
MIB = 1 << 20


def whole():
    return pl.BlockSpec(memory_space=pltpu.VMEM)


def scalars():
    return pl.BlockSpec(memory_space=pltpu.SMEM)


def params(mib):
    return pltpu.CompilerParams(vmem_limit_bytes=mib * MIB)


def pts_id(a, x, c):
    return ((a & (PLANES - 1)) * COLS + (x & (COLS - 1))) * CORES + (c & (CORES - 1))


def from_chip(block, da, dx, dc=0):
    route = [
        (pts_id(a + da, x + dx, c + dc), pts_id(a, x, c))
        for a in range(PLANES)
        for x in range(COLS)
        for c in range(CORES)
    ]
    return lax.ppermute(block, "pts", route)


def from_group(block, dz, dy):
    route = [
        ((z + dz) % ZLO * YS + (y + dy) % YS, z * YS + y) for z in range(ZLO) for y in range(YS)
    ]
    return lax.ppermute(block, "wlk", route)


def place(ids_ref):
    here = ids_ref[0]
    return here >> 3, (here >> 1) & 3, here & 1


def takes(d, a, x, c):
    low = jnp.where(x < COLS // 2, 1, 0)
    if d in ((0, 3), (1, 3)):
        return 0
    if d in ((0, 1), (1, 1)):
        return 1
    if d == (0, 2):
        return 1 - low
    if d == (1, 2):
        return low
    if d == (1, 0):
        return a
    return c


def split_columns(array, pieces, steps, mib):
    rows, cols = array.shape
    width = cols // pieces
    tile = rows // steps

    def body(x_ref, o_ref):
        for b in range(pieces):
            o_ref[b] = x_ref[:, b * width : (b + 1) * width]

    return pl.pallas_call(
        body,
        grid=(steps,),
        in_specs=[pl.BlockSpec((tile, cols), lambda i: (i, 0))],
        out_specs=pl.BlockSpec((pieces, tile, width), lambda i: (0, i, 0)),
        out_shape=jax.ShapeDtypeStruct((pieces, rows, width), array.dtype),
        compiler_params=params(mib),
    )(array)


def group_block(ids_ref, key):
    zlo, y = ids_ref[1] >> 2, ids_ref[1] & 3
    return ((zlo + key[0]) & (ZLO - 1)) * YS + ((y + key[1]) & (YS - 1))


def theta_part(ids, green_cut, blocks, rest=None):
    keys = list(blocks)
    n = len(keys)
    rows = green_cut.shape[1]
    pts = blocks[keys[0]].shape[1]
    flops = 2 * rows * pts * green_cut.shape[2] * n
    cost = pl.CostEstimate(flops=flops, bytes_accessed=flops // 600, transcendentals=0)

    if rest is None:

        def first(ids_ref, g_ref, *refs):
            cs, o_ref = refs[:n], refs[n]
            at = [group_block(ids_ref, key) for key in keys]
            o_ref[...] = sum(
                jnp.dot(g_ref[at[j]], cs[j][...], preferred_element_type=F32) for j in range(n)
            )

        return pl.pallas_call(
            first,
            in_specs=[scalars()] + [whole()] * (n + 1),
            out_specs=whole(),
            out_shape=jax.ShapeDtypeStruct((rows, pts), F32),
            cost_estimate=cost,
            compiler_params=params(10),
        )(ids, green_cut, *blocks.values())

    so_far, occ_t = rest
    elec = occ_t.shape[0]

    def last(ids_ref, g_ref, *refs):
        cs = refs[:n]
        acc_ref, occ_ref, t0_ref, t1_ref, ta_ref, tb_ref, tc_ref, ts_ref, dens_ref = refs[n:]
        at = [group_block(ids_ref, key) for key in keys]
        th_refs = (t0_ref, t1_ref)
        occ = occ_ref[...].astype(F32)
        dens = []
        for w in range(2):
            cut = pl.ds(w * elec, elec)
            t = acc_ref[cut, :] + sum(
                jnp.dot(g_ref[at[j], cut, :], cs[j][...], preferred_element_type=F32)
                for j in range(n)
            )
            t = t.astype(BF16)
            th_refs[w][0:elec, :] = t
            dens.append(jnp.sum(t.astype(F32) * occ, axis=0, keepdims=True))
        dens_ref[0:1, :] = dens[0]
        dens_ref[1:2, :] = dens[1]
        row = lax.broadcasted_iota(jnp.int32, (EXTRA, pts), 0)
        tail = jnp.where(row == 0, dens[0], jnp.where(row == 1, dens[1], 0.0)).astype(BF16)
        for w in range(2):
            th_refs[w][elec : elec + EXTRA, :] = tail
        a, x, c = place(ids_ref)
        goes = (
            takes((0, 2), a, x + 2 & 3, c),
            takes((1, 2), 1 - a, x + 2 & 3, c),
            takes((1, 0), 1 - a, x, c),
            takes((0, 0), a, x, 1 - c),
        )
        for w, o_ref in zip(goes, (ta_ref, tb_ref, tc_ref, ts_ref)):

            @pl.when(w == 0)
            def _():
                o_ref[...] = t0_ref[...]

            @pl.when(w != 0)
            def _():
                o_ref[...] = t1_ref[...]

    slab = jax.ShapeDtypeStruct((elec + EXTRA, pts), BF16)
    return pl.pallas_call(
        last,
        in_specs=[scalars()] + [whole()] * (n + 3),
        out_specs=[whole()] * 7,
        out_shape=[slab] * 6 + [jax.ShapeDtypeStruct((2, pts), F32)],
        cost_estimate=cost,
        compiler_params=params(10),
    )(ids, green_cut, *blocks.values(), so_far, occ_t)


def exchange(jobs, ids, theta_own, occ_own, kernel_cut, acc, density=None):
    n = len(jobs)
    pts, elec = occ_own.shape
    blk = kernel_cut.shape[2]

    def body(ids_ref, k_ref, *refs):
        os, ts = refs[:n], refs[n : 2 * n]
        refs = refs[2 * n :]
        to_ref, oo_ref = refs[:2]
        if density is not None:
            ex_in, pot_in, dens_ref, pot_out, vals_out, ex_ref, pot_ref, flip_ref = refs[2:]
            ex_ref[...] = ex_in[...]
            pot_ref[...] = pot_in[...]
        elif acc is None:
            ex_ref, pot_ref = refs[2:]
            ex_ref[...] = jnp.zeros_like(ex_ref)
            pot_ref[...] = jnp.zeros_like(pot_ref)
        else:
            ex_in, pot_in, ex_ref, pot_ref = refs[2:]
            ex_ref[...] = ex_in[...]
            pot_ref[...] = pot_in[...]
        a, x, c = place(ids_ref)
        for j, (chip, core, walker, _, _, weight, adds) in enumerate(jobs):
            w = takes(chip, a, x, c) if walker is None else walker
            k = k_ref[pts_id(a + chip[0], x + chip[1], c + core)].astype(F32)
            near = jnp.dot(to_ref[w], os[j][...], preferred_element_type=F32)
            far = jnp.dot(oo_ref[...], ts[j][0:elec, :], preferred_element_type=F32)
            prod = k * near * far
            ex_ref[w] += weight * jnp.sum(prod.reshape(pts // 8, 8, blk), axis=0)
            if adds:
                dens = ts[j][elec : elec + EXTRA, :].astype(F32)
                lane = lax.broadcasted_iota(jnp.int32, (pts, 128), 1)
                p0 = jnp.sum(k * dens[0:1, :], axis=1, keepdims=True)
                p1 = jnp.sum(k * dens[1:2, :], axis=1, keepdims=True)
                pot_ref[...] += jnp.where(lane == 0, p0, jnp.where(lane == 1, p1, 0.0))

        if density is not None:
            flip_ref[0:pts, :] = pot_ref[...]
            flip_ref[pts:, :] = jnp.zeros_like(flip_ref[pts:, :])
            pot = flip_ref[...].T[0:2, 0:pts]
            pot_out[...] = pot
            lane = lax.broadcasted_iota(jnp.int32, (8, 128), 1)
            vals = jnp.zeros((8, 128), F32)
            for w in range(2):
                coulomb = 0.5 * jnp.sum(dens_ref[w : w + 1, :] * pot[w : w + 1, :])
                vals = jnp.where(lane == w, coulomb, vals)
                vals = jnp.where(lane == 2 + w, -0.5 * jnp.sum(ex_ref[w]), vals)
            vals_out[...] = vals

    shapes = [jax.ShapeDtypeStruct((2, 8, blk), F32), jax.ShapeDtypeStruct((pts, 128), F32)]
    scratch = ()
    if density is not None:
        flip = pltpu.VMEM((-(-pts // 128) * 128, 128), F32)
        scratch = tuple(pltpu.VMEM(s.shape, F32) for s in shapes) + (flip,)
        shapes = [jax.ShapeDtypeStruct((2, pts), F32), jax.ShapeDtypeStruct((8, 128), F32)]
    flops = 4 * pts * blk * elec * n
    extra = () if acc is None else tuple(acc)
    if density is not None:
        extra += (density,)
    return pl.pallas_call(
        body,
        in_specs=[scalars()] + [whole()] * (2 * n + 3 + len(extra)),
        out_specs=[whole()] * 2,
        out_shape=shapes,
        scratch_shapes=scratch,
        cost_estimate=pl.CostEstimate(flops=flops, bytes_accessed=flops // 300, transcendentals=0),
        compiler_params=params(8),
    )(
        ids,
        kernel_cut,
        *[job[3] for job in jobs],
        *[job[4] for job in jobs],
        theta_own,
        occ_own,
        *extra,
    )


def everyone_total(v):
    v = v + from_chip(v, 0, 0, 1)
    r1, r2, r3 = (from_chip(v, 0, dx) for dx in (1, 2, 3))
    v = (v + r2) + (r1 + r3)
    return v + from_chip(v, 1, 0)


def local(green_half, collocation, occupied, kernel):
    walkers, elec, orb = green_half.shape
    groups = ZLO * YS
    blocks = PLANES * COLS * CORES
    ids = jnp.stack([lax.axis_index("pts"), lax.axis_index("wlk")]).astype(jnp.int32)
    occ_t = occupied.T

    coll = {(0, 0): collocation}
    coll[1, 0] = from_group(collocation, 1, 0)
    for dy in (1, 3, 2):
        coll[0, dy] = from_group(collocation, 0, dy)
    occ = {(0, 0): occ_t}
    occ[1, 0] = from_chip(occ_t, 1, 0)
    for dx in (1, 3, 2):
        occ[0, dx] = from_chip(occ_t, 0, dx)
    for dy in (1, 3, 2):
        coll[1, dy] = from_group(coll[1, 0], 0, dy)
    for dx in (1, 3, 2):
        occ[1, dx] = from_chip(occ[1, 0], 0, dx)

    green_cut = split_columns(green_half.reshape(walkers * elec, orb), groups, 4, 8)
    kernel_cut = split_columns(kernel, blocks, 5, 12)

    early = [(0, 0), (1, 0), (0, 1), (0, 3)]
    late = [(0, 2), (1, 1), (1, 3), (1, 2)]
    so_far = theta_part(ids, green_cut, {k: coll[k] for k in early})
    t0, t1, ta, tb, tc, ts, density = theta_part(
        ids, green_cut, {k: coll[k] for k in late}, rest=(so_far, occ_t)
    )
    sends = {(0, 3): t0, (1, 3): t0, (0, 1): t1, (1, 1): t1, (0, 2): ta, (1, 2): tb, (1, 0): tc}
    theta = {d: from_chip(sends[d], *d) for d in HOPS}
    theta_sib = {(0, 0): from_chip(ts, 0, 0, 1)}
    occ_sib = {d: from_chip(occ[d], 0, 0, 1) for d in [(0, 0)] + HOPS}

    t0_late, t1_late, theta_sib[0, 0] = lax.optimization_barrier((t0, t1, theta_sib[0, 0]))
    theta_own = jnp.stack([t0_late[:elec].T, t1_late[:elec].T])

    def add(jobs, acc, density=None):
        return exchange(jobs, ids, theta_own, occupied, kernel_cut, acc, density)

    acc = add([((0, 0), 0, 0, occ_t, t0, 1.0, True), ((0, 0), 0, 1, occ_t, t1, 1.0, False)], None)
    acc = add([((0, 0), 1, None, occ_sib[0, 0], theta_sib[0, 0], 2.0, True)], acc)
    for d in HOPS:
        theta_sib[d] = from_chip(theta[d], 0, 0, 1)
        acc = add([(d, 0, None, occ[d], theta[d], 2.0, True)], acc)
        acc = add(
            [(d, 1, None, occ_sib[d], theta_sib[d], 2.0, True)],
            acc,
            density if d == HOPS[-1] else None,
        )
    potential, energies = acc
    energies = everyone_total(energies)
    return potential, energies[0, :walkers], energies[0, walkers : 2 * walkers]


def solution(mesh):
    placed = (P("wlk", None, None), P("wlk", "pts"), P("pts", None), P("pts", None))

    return jax.shard_map(
        local,
        mesh=mesh,
        in_specs=placed,
        out_specs=(P("wlk", "pts"), P("wlk"), P("wlk")),
        check_vma=False,
    )
```

```python
import jax
import jax.numpy as jnp
from jax import lax
from jax.experimental import pallas as pl
from jax.experimental.pallas import tpu as pltpu
from jax.sharding import PartitionSpec as P


F32 = jnp.float32
BF16 = jnp.bfloat16
PLANES, COLS, CORES = 2, 4, 2
ZLO, YS = 2, 4
EXTRA = 8
HOPS = [(0, 3), (0, 1), (1, 0), (1, 3), (1, 1), (0, 2), (1, 2)]
MIB = 1 << 20


def whole():
    return pl.BlockSpec(memory_space=pltpu.VMEM)


def scalars():
    return pl.BlockSpec(memory_space=pltpu.SMEM)


def params(mib):
    return pltpu.CompilerParams(vmem_limit_bytes=mib * MIB)


def pts_id(a, x, c):
    return ((a & (PLANES - 1)) * COLS + (x & (COLS - 1))) * CORES + (c & (CORES - 1))


def from_chip(block, da, dx, dc=0):
    route = [
        (pts_id(a + da, x + dx, c + dc), pts_id(a, x, c))
        for a in range(PLANES)
        for x in range(COLS)
        for c in range(CORES)
    ]
    return lax.ppermute(block, "pts", route)


def from_group(block, dz, dy):
    route = [
        ((z + dz) % ZLO * YS + (y + dy) % YS, z * YS + y) for z in range(ZLO) for y in range(YS)
    ]
    return lax.ppermute(block, "wlk", route)


def place(ids_ref):
    here = ids_ref[0]
    return here >> 3, (here >> 1) & 3, here & 1


def takes(d, a, x, c):
    low = jnp.where(x < COLS // 2, 1, 0)
    if d in ((0, 3), (1, 3)):
        return 0
    if d in ((0, 1), (1, 1)):
        return 1
    if d == (0, 2):
        return 1 - low
    if d == (1, 2):
        return low
    if d == (1, 0):
        return a
    return c


def split_columns(array, pieces, steps, mib):
    rows, cols = array.shape
    width = cols // pieces
    tile = rows // steps

    def body(x_ref, o_ref):
        for b in range(pieces):
            o_ref[b] = x_ref[:, b * width : (b + 1) * width]

    return pl.pallas_call(
        body,
        grid=(steps,),
        in_specs=[pl.BlockSpec((tile, cols), lambda i: (i, 0))],
        out_specs=pl.BlockSpec((pieces, tile, width), lambda i: (0, i, 0)),
        out_shape=jax.ShapeDtypeStruct((pieces, rows, width), array.dtype),
        compiler_params=params(mib),
    )(array)


def group_block(ids_ref, key):
    zlo, y = ids_ref[1] >> 2, ids_ref[1] & 3
    return ((zlo + key[0]) & (ZLO - 1)) * YS + ((y + key[1]) & (YS - 1))


def theta_part(ids, green_cut, blocks, so_far=None, occ_t=None):
    keys = list(blocks)
    n = len(keys)
    rows = green_cut.shape[1]
    pts = blocks[keys[0]].shape[1]
    flops = 2 * rows * pts * green_cut.shape[2] * n
    cost = pl.CostEstimate(flops=flops, bytes_accessed=flops // 600, transcendentals=0)

    if occ_t is None:

        def part(ids_ref, g_ref, *refs):
            cs, o_ref = refs[:n], refs[-1]
            at = [group_block(ids_ref, key) for key in keys]
            total = sum(
                jnp.dot(g_ref[at[j]], cs[j][...], preferred_element_type=F32) for j in range(n)
            )
            o_ref[...] = total if so_far is None else refs[n][...] + total

        more = () if so_far is None else (so_far,)
        return pl.pallas_call(
            part,
            in_specs=[scalars()] + [whole()] * (n + 1 + len(more)),
            out_specs=whole(),
            out_shape=jax.ShapeDtypeStruct((rows, pts), F32),
            cost_estimate=cost,
            compiler_params=params(10),
        )(ids, green_cut, *blocks.values(), *more)

    elec = occ_t.shape[0]

    def last(ids_ref, g_ref, *refs):
        cs = refs[:n]
        acc_ref, occ_ref, t0_ref, t1_ref, ta_ref, tb_ref, tc_ref, ts_ref, dens_ref = refs[n:]
        at = [group_block(ids_ref, key) for key in keys]
        th_refs = (t0_ref, t1_ref)
        occ = occ_ref[...].astype(F32)
        dens = []
        for w in range(2):
            cut = pl.ds(w * elec, elec)
            t = acc_ref[cut, :] + sum(
                jnp.dot(g_ref[at[j], cut, :], cs[j][...], preferred_element_type=F32)
                for j in range(n)
            )
            t = t.astype(BF16)
            th_refs[w][0:elec, :] = t
            dens.append(jnp.sum(t.astype(F32) * occ, axis=0, keepdims=True))
        dens_ref[0:1, :] = dens[0]
        dens_ref[1:2, :] = dens[1]
        row = lax.broadcasted_iota(jnp.int32, (EXTRA, pts), 0)
        tail = jnp.where(row == 0, dens[0], jnp.where(row == 1, dens[1], 0.0)).astype(BF16)
        for w in range(2):
            th_refs[w][elec : elec + EXTRA, :] = tail
        a, x, c = place(ids_ref)
        goes = (
            takes((0, 2), a, x + 2 & 3, c),
            takes((1, 2), 1 - a, x + 2 & 3, c),
            takes((1, 0), 1 - a, x, c),
            takes((0, 0), a, x, 1 - c),
        )
        for w, o_ref in zip(goes, (ta_ref, tb_ref, tc_ref, ts_ref)):

            @pl.when(w == 0)
            def _():
                o_ref[...] = t0_ref[...]

            @pl.when(w != 0)
            def _():
                o_ref[...] = t1_ref[...]

    slab = jax.ShapeDtypeStruct((elec + EXTRA, pts), BF16)
    return pl.pallas_call(
        last,
        in_specs=[scalars()] + [whole()] * (n + 3),
        out_specs=[whole()] * 7,
        out_shape=[slab] * 6 + [jax.ShapeDtypeStruct((2, pts), F32)],
        cost_estimate=cost,
        compiler_params=params(10),
    )(ids, green_cut, *blocks.values(), so_far, occ_t)


def exchange(jobs, ids, theta_own, occ_own, kernel_cut, acc, density=None):
    n = len(jobs)
    elec, pts = occ_own.shape
    blk = kernel_cut.shape[2]
    contract_first = (((0,), (0,)), ((), ()))
    contract_last = (((1,), (1,)), ((), ()))

    def body(ids_ref, k_ref, *refs):
        os, ts = refs[:n], refs[n : 2 * n]
        t0_ref, t1_ref, oo_ref = refs[2 * n : 2 * n + 3]
        refs = refs[2 * n + 3 :]
        if acc is None:
            ex_ref, pot_ref = refs
            ex_ref[...] = jnp.zeros_like(ex_ref)
            pot_ref[...] = jnp.zeros_like(pot_ref)
        elif density is None:
            ex_ref, pot_ref = refs[2:]
        else:
            dens_ref, ex_ref, pot_ref, pot_out, vals_out = refs[2:]
        a, x, c = place(ids_ref)
        for j, (chip, core, walker, _, _, weight, adds) in enumerate(jobs):
            w = takes(chip, a, x, c) if walker is None else walker
            kb = k_ref[pts_id(a + chip[0], x + chip[1], c + core)]
            k = kb.astype(F32)
            dens = ts[j][elec : elec + EXTRA, :]
            far = lax.dot_general(
                oo_ref[...], ts[j][0:elec, :], contract_first, preferred_element_type=F32
            )

            if isinstance(w, int):
                own = (t0_ref, t1_ref)[w][0:elec, :]
            else:
                own = jnp.where(w == 0, t0_ref[0:elec, :], t1_ref[0:elec, :])
            near = lax.dot_general(own, os[j][...], contract_first, preferred_element_type=F32)
            prod = k * near * far
            ex_ref[w] += weight * jnp.sum(prod.reshape(pts // 8, 8, blk), axis=0)
            if adds:
                pot_ref[...] += lax.dot_general(
                    dens, kb, contract_last, preferred_element_type=F32
                )
        if density is not None:
            pot = pot_ref[0:2, :]
            pot_out[...] = pot
            lane = lax.broadcasted_iota(jnp.int32, (8, 128), 1)
            vals = jnp.zeros((8, 128), F32)
            for w in range(2):
                coulomb = 0.5 * jnp.sum(dens_ref[w : w + 1, :] * pot[w : w + 1, :])
                vals = jnp.where(lane == w, coulomb, vals)
                vals = jnp.where(lane == 2 + w, -0.5 * jnp.sum(ex_ref[w]), vals)
            vals_out[...] = vals

    shapes = [jax.ShapeDtypeStruct((2, 8, blk), F32), jax.ShapeDtypeStruct((EXTRA, pts), F32)]
    flops = 4 * pts * blk * elec * n
    operands = [ids, kernel_cut] + [job[3] for job in jobs] + [job[4] for job in jobs]
    operands += [*theta_own, occ_own]
    alias = {}
    if acc is not None:
        alias = {len(operands): 0, len(operands) + 1: 1}
        operands += acc
    if density is not None:
        operands += [density]
        shapes += [jax.ShapeDtypeStruct((2, pts), F32), jax.ShapeDtypeStruct((8, 128), F32)]
    return pl.pallas_call(
        body,
        in_specs=[scalars()] + [whole()] * (len(operands) - 1),
        out_specs=[whole()] * len(shapes),
        out_shape=shapes,
        input_output_aliases=alias,
        cost_estimate=pl.CostEstimate(flops=flops, bytes_accessed=flops // 300, transcendentals=0),
        compiler_params=params(8),
    )(*operands)


def everyone_total(v):
    v = v + from_chip(v, 0, 0, 1)
    r1, r2, r3 = (from_chip(v, 0, dx) for dx in (1, 2, 3))
    v = (v + r2) + (r1 + r3)
    return v + from_chip(v, 1, 0)


def local(green_half, collocation, occupied, kernel):
    walkers, elec, orb = green_half.shape
    groups = ZLO * YS
    blocks = PLANES * COLS * CORES
    ids = jnp.stack([lax.axis_index("pts"), lax.axis_index("wlk")]).astype(jnp.int32)
    occ_t = occupied.T

    coll = {(0, 0): collocation}
    coll[1, 0] = from_group(collocation, 1, 0)
    for dy in (2, 1, 3):
        coll[0, dy] = from_group(collocation, 0, dy)
    occ = {(0, 0): occ_t}
    occ[1, 0] = from_chip(occ_t, 1, 0)
    for dx in (1, 3, 2):
        occ[0, dx] = from_chip(occ_t, 0, dx)
    for dy in (1, 3):
        coll[1, dy] = from_group(coll[1, 0], 0, dy)
    coll[1, 2] = from_group(coll[0, 2], 1, 0)
    for dx in (1, 3, 2):
        occ[1, dx] = from_chip(occ[1, 0], 0, dx)

    green_cut = split_columns(green_half.reshape(walkers * elec, orb), groups, 4, 8)
    kernel_cut = split_columns(kernel, blocks, 5, 12)

    def some(keys):
        return {k: coll[k] for k in keys}

    so_far = theta_part(ids, green_cut, some([(0, 0), (1, 0), (0, 2), (0, 1), (0, 3)]))
    so_far = theta_part(ids, green_cut, some([(1, 1), (1, 3)]), so_far)
    t0, t1, ta, tb, tc, ts, density = theta_part(ids, green_cut, some([(1, 2)]), so_far, occ_t)
    sends = {(0, 3): t0, (1, 3): t0, (0, 1): t1, (1, 1): t1, (0, 2): ta, (1, 2): tb, (1, 0): tc}
    theta = {d: from_chip(sends[d], *d) for d in HOPS}
    theta_sib = {(0, 0): from_chip(ts, 0, 0, 1)}
    occ_sib = {d: from_chip(occ[d], 0, 0, 1) for d in [(0, 0)] + HOPS}

    theta_own = (t0, t1)

    def add(jobs, acc, density=None):
        return exchange(jobs, ids, theta_own, occ_t, kernel_cut, acc, density)

    acc = add([((0, 0), 0, 0, occ_t, t0, 1.0, True), ((0, 0), 0, 1, occ_t, t1, 1.0, False)], None)
    acc = add([((0, 0), 1, None, occ_sib[0, 0], theta_sib[0, 0], 2.0, True)], acc)
    for d in HOPS:
        theta_sib[d] = from_chip(theta[d], 0, 0, 1)
        acc = add([(d, 0, None, occ[d], theta[d], 2.0, True)], acc)
        acc = add(
            [(d, 1, None, occ_sib[d], theta_sib[d], 2.0, True)],
            acc,
            density if d == HOPS[-1] else None,
        )
    _, _, potential, energies = acc
    energies = everyone_total(energies)
    return potential, energies[0, :walkers], energies[0, walkers : 2 * walkers]


def solution(mesh):
    placed = (P("wlk", None, None), P("wlk", "pts"), P("pts", None), P("pts", None))

    return jax.shard_map(
        local,
        mesh=mesh,
        in_specs=placed,
        out_specs=(P("wlk", "pts"), P("wlk"), P("wlk")),
        check_vma=False,
    )
```

```python
import jax
import jax.numpy as jnp
from jax import lax
from jax.experimental import pallas as pl
from jax.experimental.pallas import tpu as pltpu
from jax.sharding import PartitionSpec as P


F32 = jnp.float32
BF16 = jnp.bfloat16
PLANES, COLS, CORES = 2, 4, 2
ZLO, YS = 2, 4
EXTRA = 8
SLOTS = {
    "left": ((0, 3), (0, 3)),
    "right": ((0, 1), (0, 1)),
    "plane": ((1, 0), (1, 0)),
    "side": ((1, 1), (1, 3)),
    "far": ((0, 2), (1, 2)),
    "side2": ((1, 3), (1, 1)),
    "far2": ((1, 2), (0, 2)),
}
SWAPPED = {"side": "side2", "far": "far2"}
MIB = 1 << 20


def whole():
    return pl.BlockSpec(memory_space=pltpu.VMEM)


def scalars():
    return pl.BlockSpec(memory_space=pltpu.SMEM)


def params(mib):
    return pltpu.CompilerParams(vmem_limit_bytes=mib * MIB)


def pts_id(a, x, c):
    return ((a & (PLANES - 1)) * COLS + (x & (COLS - 1))) * CORES + (c & (CORES - 1))


def from_device(block, source):
    route = []
    for a in range(PLANES):
        for x in range(COLS):
            for c in range(CORES):
                for z in range(ZLO):
                    for y in range(YS):
                        sa, sx, sc, sz, sy = source(a, x, c, z, y)
                        start = pts_id(sa, sx, sc) * ZLO * YS + (sz & 1) * YS + (sy & 3)
                        route.append((start, pts_id(a, x, c) * ZLO * YS + z * YS + y))
    return lax.ppermute(block, ("pts", "wlk"), route)


def from_chip(block, da, dx, dc=0):
    return from_device(block, lambda a, x, c, z, y: (a + da, x + dx, c + dc, z, y))


def from_group(block, dz, dy):
    return from_device(block, lambda a, x, c, z, y: (a, x, c, z + dz, y + dy))


def from_slot(block, slot, columns_only=False):
    def source(a, x, c, z, y):
        da, dx = SLOTS[slot][(y ^ c) & 1]
        return (a if columns_only else a + da), x + dx, c, z, y

    return from_device(block, source)


def place(ids_ref):
    here = ids_ref[0]
    return here >> 3, (here >> 1) & 3, here & 1, ids_ref[1] & 3


def takes(slot, a, x, c, odd):
    low = jnp.where((x & 3) < COLS // 2, 1, 0)
    return {
        "own": c,
        "left": 0,
        "right": 1,
        "plane": a,
        "side": 1 - odd,
        "side2": odd,
        "far": jnp.where(odd == 1, low, 1 - low),
        "far2": jnp.where(odd == 1, 1 - low, low),
    }[slot]


def chip_of(slot, a, x, odd):
    (a0, x0), (a1, x1) = SLOTS.get(slot, ((0, 0), (0, 0)))
    return a + jnp.where(odd == 1, a1, a0), x + jnp.where(odd == 1, x1, x0)


def split_columns(array, pieces, steps, mib):
    rows, cols = array.shape
    width = cols // pieces
    tile = rows // steps

    def body(x_ref, o_ref):
        for b in range(pieces):
            o_ref[b] = x_ref[:, b * width : (b + 1) * width]

    return pl.pallas_call(
        body,
        grid=(steps,),
        in_specs=[pl.BlockSpec((tile, cols), lambda i: (i, 0))],
        out_specs=pl.BlockSpec((pieces, tile, width), lambda i: (0, i, 0)),
        out_shape=jax.ShapeDtypeStruct((pieces, rows, width), array.dtype),
        compiler_params=params(mib),
    )(array)


def group_block(ids_ref, key):
    zlo, y = ids_ref[1] >> 2, ids_ref[1] & 3
    return ((zlo + key[0]) & (ZLO - 1)) * YS + ((y + key[1]) & (YS - 1))


def theta_part(ids, green_cut, blocks, so_far=None, occ_t=None):
    keys = list(blocks)
    n = len(keys)
    rows = green_cut.shape[1]
    pts = blocks[keys[0]].shape[1]
    flops = 2 * rows * pts * green_cut.shape[2] * n
    cost = pl.CostEstimate(flops=flops, bytes_accessed=flops // 600, transcendentals=0)

    if occ_t is None:

        def part(ids_ref, g_ref, *refs):
            cs, o_ref = refs[:n], refs[-1]
            at = [group_block(ids_ref, key) for key in keys]
            total = sum(
                jnp.dot(g_ref[at[j]], cs[j][...], preferred_element_type=F32) for j in range(n)
            )
            o_ref[...] = total if so_far is None else refs[n][...] + total

        more = () if so_far is None else (so_far,)
        return pl.pallas_call(
            part,
            in_specs=[scalars()] + [whole()] * (n + 1 + len(more)),
            out_specs=whole(),
            out_shape=jax.ShapeDtypeStruct((rows, pts), F32),
            cost_estimate=cost,
            compiler_params=params(10),
        )(ids, green_cut, *blocks.values(), *more)

    elec = occ_t.shape[0]

    def last(ids_ref, g_ref, *refs):
        cs = refs[:n]
        acc_ref, occ_ref, t0_ref, t1_ref, *pick_refs, dens_ref = refs[n:]
        at = [group_block(ids_ref, key) for key in keys]
        th_refs = (t0_ref, t1_ref)
        occ = occ_ref[...].astype(F32)
        dens = []
        for w in range(2):
            cut = pl.ds(w * elec, elec)
            t = acc_ref[cut, :] + sum(
                jnp.dot(g_ref[at[j], cut, :], cs[j][...], preferred_element_type=F32)
                for j in range(n)
            )
            t = t.astype(BF16)
            th_refs[w][0:elec, :] = t
            dens.append(jnp.sum(t.astype(F32) * occ, axis=0, keepdims=True))
        dens_ref[0:1, :] = dens[0]
        dens_ref[1:2, :] = dens[1]
        row = lax.broadcasted_iota(jnp.int32, (EXTRA, pts), 0)
        tail = jnp.where(row == 0, dens[0], jnp.where(row == 1, dens[1], 0.0)).astype(BF16)
        for w in range(2):
            th_refs[w][elec : elec + EXTRA, :] = tail
        a, x, c, y = place(ids_ref)
        odd = (y ^ c) & 1
        goes = (
            takes("plane", 1 - a, x, c, odd),
            takes("side", a, x, c, odd),
            takes("far", a, x + 2, c, odd),
            takes("side2", a, x, c, odd),
            takes("far2", a, x + 2, c, odd),
            takes("own", a, x, 1 - c, odd),
        )
        for w, o_ref in zip(goes, pick_refs):

            @pl.when(w == 0)
            def _():
                o_ref[...] = t0_ref[...]

            @pl.when(w != 0)
            def _():
                o_ref[...] = t1_ref[...]

    slab = jax.ShapeDtypeStruct((elec + EXTRA, pts), BF16)
    return pl.pallas_call(
        last,
        in_specs=[scalars()] + [whole()] * (n + 3),
        out_specs=[whole()] * 9,
        out_shape=[slab] * 8 + [jax.ShapeDtypeStruct((2, pts), F32)],
        cost_estimate=cost,
        compiler_params=params(10),
    )(ids, green_cut, *blocks.values(), so_far, occ_t)


def exchange(jobs, ids, theta_own, occ_own, kernel_cut, acc, density=None):
    n = len(jobs)
    elec, pts = occ_own.shape
    blk = kernel_cut.shape[2]
    contract_first = (((0,), (0,)), ((), ()))
    contract_last = (((1,), (1,)), ((), ()))

    def body(ids_ref, k_ref, *refs):
        os, ts = refs[:n], refs[n : 2 * n]
        t0_ref, t1_ref, oo_ref = refs[2 * n : 2 * n + 3]
        refs = refs[2 * n + 3 :]
        if acc is None:
            ex_ref, pot_ref = refs
            ex_ref[...] = jnp.zeros_like(ex_ref)
            pot_ref[...] = jnp.zeros_like(pot_ref)
        elif density is None:
            ex_ref, pot_ref = refs[2:]
        else:
            dens_ref, ex_ref, pot_ref, pot_out, vals_out = refs[2:]
        a, x, c, y = place(ids_ref)
        for j, (slot, core, walker, _, _, weight, adds) in enumerate(jobs):
            odd = (y ^ c ^ core) & 1
            w = takes(slot, a, x, c, odd) if walker is None else walker
            kb = k_ref[pts_id(*chip_of(slot, a, x, odd), c + core)]
            k = kb.astype(F32)
            dens = ts[j][elec : elec + EXTRA, :]
            far = lax.dot_general(
                oo_ref[...], ts[j][0:elec, :], contract_first, preferred_element_type=F32
            )

            if isinstance(w, int):
                own = (t0_ref, t1_ref)[w][0:elec, :]
            else:
                own = jnp.where(w == 0, t0_ref[0:elec, :], t1_ref[0:elec, :])
            near = lax.dot_general(own, os[j][...], contract_first, preferred_element_type=F32)
            prod = k * near * far
            ex_ref[w] += weight * jnp.sum(prod.reshape(pts // 8, 8, blk), axis=0)
            if adds:
                pot_ref[...] += lax.dot_general(
                    dens, kb, contract_last, preferred_element_type=F32
                )
        if density is not None:
            pot = pot_ref[0:2, :]
            pot_out[...] = pot
            lane = lax.broadcasted_iota(jnp.int32, (8, 128), 1)
            vals = jnp.zeros((8, 128), F32)
            for w in range(2):
                coulomb = 0.5 * jnp.sum(dens_ref[w : w + 1, :] * pot[w : w + 1, :])
                vals = jnp.where(lane == w, coulomb, vals)
                vals = jnp.where(lane == 2 + w, -0.5 * jnp.sum(ex_ref[w]), vals)
            vals_out[...] = vals

    shapes = [jax.ShapeDtypeStruct((2, 8, blk), F32), jax.ShapeDtypeStruct((EXTRA, pts), F32)]
    flops = 4 * pts * blk * elec * n
    operands = [ids, kernel_cut] + [job[3] for job in jobs] + [job[4] for job in jobs]
    operands += [*theta_own, occ_own]
    alias = {}
    if acc is not None:
        alias = {len(operands): 0, len(operands) + 1: 1}
        operands += acc
    if density is not None:
        operands += [density]
        shapes += [jax.ShapeDtypeStruct((2, pts), F32), jax.ShapeDtypeStruct((8, 128), F32)]
    return pl.pallas_call(
        body,
        in_specs=[scalars()] + [whole()] * (len(operands) - 1),
        out_specs=[whole()] * len(shapes),
        out_shape=shapes,
        input_output_aliases=alias,
        cost_estimate=pl.CostEstimate(flops=flops, bytes_accessed=flops // 300, transcendentals=0),
        compiler_params=params(8),
    )(*operands)


def everyone_total(v):
    v = v + from_chip(v, 0, 0, 1)
    r1, r2, r3 = (from_chip(v, 0, dx) for dx in (1, 2, 3))
    v = (v + r2) + (r1 + r3)
    return v + from_chip(v, 1, 0)


def local(green_half, collocation, occupied, kernel):
    walkers, elec, orb = green_half.shape
    groups = ZLO * YS
    blocks = PLANES * COLS * CORES
    ids = jnp.stack([lax.axis_index("pts"), lax.axis_index("wlk")]).astype(jnp.int32)
    occ_t = occupied.T

    coll = {(0, 0): collocation}
    coll[1, 0] = from_group(collocation, 1, 0)
    for dy in (2, 1, 3):
        coll[0, dy] = from_group(collocation, 0, dy)
    for dy in (1, 3):
        coll[1, dy] = from_group(coll[1, 0], 0, dy)
    coll[1, 2] = from_group(coll[0, 2], 1, 0)
    occ = {slot: from_slot(occ_t, slot) for slot in ("left", "right", "plane")}
    here_odd = (ids[1] ^ ids[0]) & 1
    occ_far = jnp.where(here_odd == 1, occ["plane"], occ_t)
    occ["side"] = from_slot(occ["plane"], "side", True)
    occ["far"] = from_slot(occ_far, "far", True)
    for slot, slot2 in SWAPPED.items():
        occ[slot2] = from_device(occ[slot], lambda a, x, c, z, y: (a, x, c, z, y ^ 1))

    green_cut = split_columns(green_half.reshape(walkers * elec, orb), groups, 4, 8)
    kernel_cut = split_columns(kernel, blocks, 5, 12)

    def some(keys):
        return {k: coll[k] for k in keys}

    so_far = theta_part(ids, green_cut, some([(0, 0), (1, 0), (0, 2), (0, 1), (0, 3)]))
    so_far = theta_part(ids, green_cut, some([(1, 1), (1, 3)]), so_far)
    t0, t1, *picks, t_sib, density = theta_part(ids, green_cut, some([(1, 2)]), so_far, occ_t)
    sends = dict(zip(SLOTS, (t0, t1, *picks)))
    theta = {slot: from_slot(sends[slot], slot) for slot in SLOTS}
    theta_sib = {"own": from_chip(t_sib, 0, 0, 1)}
    occ["own"] = occ_t
    occ_sib = {slot: from_chip(occ[slot], 0, 0, 1) for slot in ("own", *SLOTS)}

    theta_own = (t0, t1)

    def add(jobs, acc, density=None):
        return exchange(jobs, ids, theta_own, occ_t, kernel_cut, acc, density)

    acc = add([("own", 0, 0, occ_t, t0, 1.0, True), ("own", 0, 1, occ_t, t1, 1.0, False)], None)
    acc = add([("own", 1, None, occ_sib["own"], theta_sib["own"], 2.0, True)], acc)
    for slot in SLOTS:
        theta_sib[slot] = from_chip(theta[slot], 0, 0, 1)
        acc = add([(slot, 0, None, occ[slot], theta[slot], 2.0, True)], acc)
        acc = add(
            [(slot, 1, None, occ_sib[slot], theta_sib[slot], 2.0, True)],
            acc,
            density if slot == list(SLOTS)[-1] else None,
        )
    _, _, potential, energies = acc
    energies = everyone_total(energies)
    return potential, energies[0, :walkers], energies[0, walkers : 2 * walkers]


def solution(mesh):
    placed = (P("wlk", None, None), P("wlk", "pts"), P("pts", None), P("pts", None))

    return jax.shard_map(
        local,
        mesh=mesh,
        in_specs=placed,
        out_specs=(P("wlk", "pts"), P("wlk"), P("wlk")),
        check_vma=False,
    )
```

```python
import jax
import jax.numpy as jnp
from jax import lax
from jax.experimental import pallas as pl
from jax.experimental.pallas import tpu as pltpu
from jax.sharding import PartitionSpec as P


F32 = jnp.float32
BF16 = jnp.bfloat16
PLANES, COLS, CORES = 2, 4, 2
ZLO, YS = 2, 4
EXTRA = 8
SLOTS = {
    "left": ((0, 3), (0, 3)),
    "right": ((0, 1), (0, 1)),
    "far": ((0, 2), (0, 2)),
    "side": ((1, 3), (1, 1)),
    "plane": ((1, 0), (1, 0)),
    "side2": ((1, 1), (1, 3)),
    "far2": ((1, 2), (1, 2)),
}
MIB = 1 << 20


def whole():
    return pl.BlockSpec(memory_space=pltpu.VMEM)


def scalars():
    return pl.BlockSpec(memory_space=pltpu.SMEM)


def params(mib):
    return pltpu.CompilerParams(vmem_limit_bytes=mib * MIB)


def pts_id(a, x, c):
    return ((a & (PLANES - 1)) * COLS + (x & (COLS - 1))) * CORES + (c & (CORES - 1))


def from_device(block, source):
    route = []
    for a in range(PLANES):
        for x in range(COLS):
            for c in range(CORES):
                for z in range(ZLO):
                    for y in range(YS):
                        sa, sx, sc, sz, sy = source(a, x, c, z, y)
                        start = pts_id(sa, sx, sc) * ZLO * YS + (sz & 1) * YS + (sy & 3)
                        route.append((start, pts_id(a, x, c) * ZLO * YS + z * YS + y))
    return lax.ppermute(block, ("pts", "wlk"), route)


def from_chip(block, da, dx, dc=0):
    return from_device(block, lambda a, x, c, z, y: (a + da, x + dx, c + dc, z, y))


def from_group(block, dz, dy):
    return from_device(block, lambda a, x, c, z, y: (a, x, c, z + dz, y + dy))


def from_column(block, slot):
    def source(a, x, c, z, y):
        return a, x + SLOTS[slot][(y ^ c) & 1][1], c, z, y

    return from_device(block, source)


def place(ids_ref):
    here = ids_ref[0]
    return here >> 3, (here >> 1) & 3, here & 1, ids_ref[1] & 3


def takes(slot, a, x, c, odd):
    low = jnp.where((x & 3) < COLS // 2, 1, 0)
    return {
        "own": c,
        "left": 0,
        "right": 1,
        "far": 1 - low,
        "side": odd,
        "plane": a,
        "side2": 1 - odd,
        "far2": low,
    }[slot]


def chip_of(slot, a, x, odd):
    (a0, x0), (a1, x1) = SLOTS.get(slot, ((0, 0), (0, 0)))
    return a + jnp.where(odd == 1, a1, a0), x + jnp.where(odd == 1, x1, x0)


def split_columns(array, pieces, steps, mib, room=1):
    rows, cols = array.shape
    width = cols // pieces
    tile = rows // steps

    def body(x_ref, o_ref):
        @pl.loop(0, tile // 40)
        def _(part):
            cut = pl.ds(pl.multiple_of(part * 40, 8), 40)
            for b in range(pieces):
                o_ref[b, cut, :] = x_ref[cut, b * width : (b + 1) * width]

    return pl.pallas_call(
        body,
        grid=(steps,),
        in_specs=[pl.BlockSpec((tile, cols), lambda i: (i, 0))],
        out_specs=pl.BlockSpec((pieces, tile, width), lambda i: (0, i, 0)),
        out_shape=jax.ShapeDtypeStruct((pieces * room, rows, width), array.dtype),
        compiler_params=params(mib),
    )(array)


def pick(ids, takes_second, one, two):
    def body(ids_ref, one_ref, two_ref, o_ref):
        second = takes_second(*place(ids_ref))

        @pl.when(second == 0)
        def _():
            o_ref[...] = one_ref[...]

        @pl.when(second != 0)
        def _():
            o_ref[...] = two_ref[...]

    return pl.pallas_call(
        body,
        in_specs=[scalars(), whole(), whole()],
        out_specs=whole(),
        out_shape=jax.ShapeDtypeStruct(one.shape, one.dtype),
        compiler_params=params(4),
    )(ids, one, two)


def group_block(ids_ref, key):
    zlo, y = ids_ref[1] >> 2, ids_ref[1] & 3
    return ((zlo + key[0]) & (ZLO - 1)) * YS + ((y + key[1]) & (YS - 1))


def theta_part(ids, green_cut, blocks, so_far=None, occ_t=None):
    keys = list(blocks)
    n = len(keys)
    rows = green_cut.shape[1]
    pts = blocks[keys[0]].shape[1]
    flops = 2 * rows * pts * green_cut.shape[2] * n
    cost = pl.CostEstimate(flops=flops, bytes_accessed=flops // 600, transcendentals=0)

    if occ_t is None:

        def part(ids_ref, g_ref, *refs):
            cs, o_ref = refs[:n], refs[-1]
            at = [group_block(ids_ref, key) for key in keys]

            @pl.loop(0, 2)
            def _(half):
                cut = pl.ds(pl.multiple_of(half * (rows // 2), 8), rows // 2)
                total = sum(
                    jnp.dot(g_ref[at[j], cut, :], cs[j][...], preferred_element_type=F32)
                    for j in range(n)
                )
                o_ref[cut, :] = total if so_far is None else refs[n][cut, :] + total

        more = () if so_far is None else (so_far,)
        return pl.pallas_call(
            part,
            in_specs=[scalars()] + [whole()] * (n + 1 + len(more)),
            out_specs=whole(),
            out_shape=jax.ShapeDtypeStruct((rows, pts), F32),
            cost_estimate=cost,
            compiler_params=params(8),
        )(ids, green_cut, *blocks.values(), *more)

    elec = occ_t.shape[0]

    def last(ids_ref, g_ref, *refs):
        cs = refs[:n]
        acc_ref, occ_ref, t0_ref, t1_ref, *pick_refs, dens_ref = refs[n:]
        at = [group_block(ids_ref, key) for key in keys]
        th_refs = (t0_ref, t1_ref)
        occ = occ_ref[...].astype(F32)
        dens = []
        for w in range(2):
            cut = pl.ds(w * elec, elec)
            t = acc_ref[cut, :] + sum(
                jnp.dot(g_ref[at[j], cut, :], cs[j][...], preferred_element_type=F32)
                for j in range(n)
            )
            t = t.astype(BF16)
            th_refs[w][0:elec, :] = t
            dens.append(jnp.sum(t.astype(F32) * occ, axis=0, keepdims=True))
        dens_ref[0:1, :] = dens[0]
        dens_ref[1:2, :] = dens[1]
        row = lax.broadcasted_iota(jnp.int32, (EXTRA, pts), 0)
        tail = jnp.where(row == 0, dens[0], jnp.where(row == 1, dens[1], 0.0)).astype(BF16)
        for w in range(2):
            th_refs[w][elec : elec + EXTRA, :] = tail
        a, x, c, y = place(ids_ref)
        odd = (y ^ c) & 1
        goes = (
            odd,
            1 - odd,
            takes("far", a, x + 2, c, odd),
            takes("own", a, x, 1 - c, odd),
        )
        for w, o_ref in zip(goes, pick_refs):

            @pl.when(w == 0)
            def _():
                o_ref[...] = t0_ref[...]

            @pl.when(w != 0)
            def _():
                o_ref[...] = t1_ref[...]

    slab = jax.ShapeDtypeStruct((elec + EXTRA, pts), BF16)
    return pl.pallas_call(
        last,
        in_specs=[scalars()] + [whole()] * (n + 3),
        out_specs=[whole()] * 7,
        out_shape=[slab] * 6 + [jax.ShapeDtypeStruct((2, pts), F32)],
        cost_estimate=cost,
        compiler_params=params(8),
    )(ids, green_cut, *blocks.values(), so_far, occ_t)


def exchange(jobs, ids, own, kernel_cut, acc=None, density=None):
    n = len(jobs)
    elec, pts = jobs[0][3][0].shape
    contract_last = (((1,), (1,)), ((), ()))
    occ_blocks, occ_first = [], []
    for job in jobs:
        occ_first.append(len(occ_blocks))
        occ_blocks += job[3]
    first = acc is None

    def body(ids_ref, k_ref, *refs):
        refs = list(refs)
        os = [refs.pop(0) for _ in occ_blocks]
        ts = [refs.pop(0) for _ in jobs]
        block_ref, near_ref, far_ref, sem, *flip_ref = refs[-5:] if first else refs[-4:]
        if first:
            ex_ref, pot_ref, own_ref = refs[:3]
            ex_ref[...] = jnp.zeros_like(ex_ref)
            pot_ref[...] = jnp.zeros_like(pot_ref)
        else:
            own_ref = refs[0]
            dens_ref, ex_ref, pot_ref, pot_out, vals_out = (
                (None, *refs[3:5], None, None) if density is None else refs[3:8]
            )
        a, x, c, y = place(ids_ref)

        def of_job(j, values):
            value = values[0]
            for i in range(1, n):
                value = jnp.where(j == i, values[i], value)
            return value

        starts, walkers, occ_at = [], [], []
        for (slot, core, walker, blocks, *_), at in zip(jobs, occ_first):
            odd = (y ^ c ^ core) & 1
            walkers.append(takes(slot, a, x, c, odd) if walker is None else walker)
            starts.append(pts_id(*chip_of(slot, a, x, odd), c + core))
            occ_at.append(at + odd if len(blocks) > 1 else at)

        def copy(j, block):
            return pltpu.make_async_copy(k_ref.at[block], block_ref.at[j], sem.at[j])

        for j in range(n):
            copy(j, starts[j]).start()
        if first:
            for to, block in enumerate((ts[0], ts[1], os[0])):
                flip_ref[0][0:elec, 0:pts] = block[0:elec, :].astype(F32)
                own_ref[to] = flip_ref[0][...].T[0:pts, 0:elec].astype(BF16)

        @pl.loop(0, n)
        def _(j):
            w = of_job(j, walkers)
            at = of_job(j, occ_at)
            occ, theta = os[0][...], ts[0][...]
            for i in range(1, len(os)):
                occ = jnp.where(at == i, os[i][...], occ)
            for i in range(1, n):
                theta = jnp.where(j == i, ts[i][...], theta)
            near_ref[...] = jnp.dot(own_ref[w], occ, preferred_element_type=F32)
            far_ref[...] = jnp.dot(own_ref[2], theta[0:elec, :], preferred_element_type=F32)
            copy(j, 0).wait()
            k = block_ref[j]
            prod = k.astype(F32) * near_ref[...] * far_ref[...]
            weight = of_job(j, [job[5] for job in jobs])
            ex_ref[w] += weight * jnp.sum(prod.reshape(pts // 8, 8, pts), axis=0)
            adds = of_job(j, [1.0 if job[6] else 0.0 for job in jobs])
            pot_ref[...] += adds * lax.dot_general(
                theta[elec : elec + EXTRA, :],
                k,
                contract_last,
                preferred_element_type=F32,
            )

        if density is not None:
            pot = pot_ref[0:2, :]
            pot_out[...] = pot
            lane = lax.broadcasted_iota(jnp.int32, (8, 128), 1)
            vals = jnp.zeros((8, 128), F32)
            for w in range(2):
                coulomb = 0.5 * jnp.sum(dens_ref[w : w + 1, :] * pot[w : w + 1, :])
                vals = jnp.where(lane == w, coulomb, vals)
                vals = jnp.where(lane == 2 + w, -0.5 * jnp.sum(ex_ref[w]), vals)
            vals_out[...] = vals

    shapes = [jax.ShapeDtypeStruct((2, 8, pts), F32), jax.ShapeDtypeStruct((EXTRA, pts), F32)]
    flops = 4 * pts * pts * elec * n
    operands = [ids, kernel_cut] + occ_blocks + [job[4] for job in jobs]
    scratch = [
        pltpu.VMEM((n, pts, pts), BF16),
        pltpu.VMEM((pts, pts), F32),
        pltpu.VMEM((pts, pts), F32),
        pltpu.SemaphoreType.DMA((n,)),
    ]
    alias = {}
    if first:
        shapes += [jax.ShapeDtypeStruct((3, pts, elec), BF16)]
        scratch += [pltpu.VMEM((-(-elec // 128) * 128, -(-pts // 128) * 128), F32)]
    else:
        operands += [own]
        alias = {len(operands): 0, len(operands) + 1: 1}
        operands += acc
    if density is not None:
        operands += [density]
        shapes += [jax.ShapeDtypeStruct((2, pts), F32), jax.ShapeDtypeStruct((8, 128), F32)]
    return pl.pallas_call(
        body,
        in_specs=[scalars(), pl.BlockSpec(memory_space=pl.ANY)]
        + [whole()] * (len(operands) - 2),
        out_specs=[whole()] * len(shapes),
        out_shape=shapes,
        scratch_shapes=scratch,
        input_output_aliases=alias,
        cost_estimate=pl.CostEstimate(flops=flops, bytes_accessed=flops // 300, transcendentals=0),
        compiler_params=params(9),
    )(*operands)


def everyone_total(v):
    v = v + from_chip(v, 0, 0, 1)
    r1, r2, r3 = (from_chip(v, 0, dx) for dx in (1, 2, 3))
    v = (v + r2) + (r1 + r3)
    return v + from_chip(v, 1, 0)


def local(green_half, collocation, occupied, kernel):
    walkers, elec, orb = green_half.shape
    groups = ZLO * YS
    ids = jnp.stack([lax.axis_index("pts"), lax.axis_index("wlk")]).astype(jnp.int32)
    occ_t = occupied.T

    coll = {(0, 0): collocation}
    coll[1, 0] = from_group(collocation, 1, 0)
    for dy in (2, 1, 3):
        coll[0, dy] = from_group(collocation, 0, dy)
    for dy in (1, 3):
        coll[1, dy] = from_group(coll[1, 0], 0, dy)
    coll[1, 2] = from_group(coll[0, 2], 1, 0)
    occ_left = from_column(occ_t, "left")
    occ_right = from_column(occ_t, "right")
    occ_plane = from_chip(occ_t, 1, 0)
    occ_side = from_column(occ_plane, "side")
    occ_pick = pick(ids, lambda a, x, c, y: (y ^ c) & 1, occ_t, occ_plane)
    occ_far = from_column(occ_pick, "far")

    def from_y(block):
        return from_device(block, lambda a, x, c, z, y: (a, x, c, z, y ^ 1))

    occ_side2 = from_y(occ_side)
    occ_far2 = from_y(occ_far)
    occ = {"own": [occ_t], "left": [occ_left], "right": [occ_right], "far": [occ_far, occ_far2]}
    occ |= {"side": [occ_side], "plane": [occ_plane], "side2": [occ_side2]}

    green_cut = split_columns(green_half.reshape(walkers * elec, orb), groups, 4, 8)

    kernel_cut = split_columns(kernel, PLANES * COLS * CORES, 15, 6, 5)

    def some(keys):
        return {k: coll[k] for k in keys}

    so_far = theta_part(ids, green_cut, some([(0, 0), (1, 0), (0, 2)]))
    so_far = theta_part(ids, green_cut, some([(0, 1), (0, 3), (1, 1), (1, 3)]), so_far)
    t0, t1, t_first, t_second, t_far, t_sib, density = theta_part(
        ids, green_cut, some([(1, 2)]), so_far, occ_t
    )
    first = from_chip(t_first, 1, 0)
    second = from_chip(t_second, 1, 0)
    plane = pick(ids, lambda a, x, c, y: a ^ (y ^ c) & 1, first, second)
    far2 = pick(ids, lambda a, x, c, y: x >> 1 ^ (y ^ c) & 1, first, second)
    theta = {
        "left": from_column(t0, "left"),
        "right": from_column(t1, "right"),
        "far": from_column(t_far, "far"),
        "side": from_column(first, "side"),
        "plane": plane,
        "side2": from_column(second, "side2"),
        "far2": from_column(far2, "far2"),
    }
    theta_sib = {"own": from_chip(t_sib, 0, 0, 1)}
    occ_sib = {slot: [from_chip(block, 0, 0, 1) for block in occ[slot][:1]] for slot in occ}
    occ_sib["far"] += [from_chip(occ_far2, 0, 0, 1)]
    for known in (occ, occ_sib):
        known["far2"] = known["far"][::-1]
    *acc, own = exchange(
        [
            ("own", 0, 0, [occ_t], t0, 1.0, True),
            ("own", 0, 1, [occ_t], t1, 1.0, False),
            ("own", 1, None, occ_sib["own"], theta_sib["own"], 2.0, True),
        ],
        ids,
        None,
        kernel_cut,
    )
    for slot in SLOTS:
        theta_sib[slot] = from_chip(theta[slot], 0, 0, 1)
        same = (slot, 0, None, occ[slot], theta[slot], 2.0, True)
        sib = (slot, 1, None, occ_sib[slot], theta_sib[slot], 2.0, True)
        if slot == list(SLOTS)[-1]:
            acc = exchange([same], ids, own, kernel_cut, acc)
            acc = exchange([sib], ids, own, kernel_cut, acc, density)
        else:
            acc = exchange([same, sib], ids, own, kernel_cut, acc)
    _, _, potential, energies = acc
    energies = everyone_total(energies)
    return potential, energies[0, :walkers], energies[0, walkers : 2 * walkers]


def solution(mesh):
    placed = (P("wlk", None, None), P("wlk", "pts"), P("pts", None), P("pts", None))

    return jax.shard_map(
        local,
        mesh=mesh,
        in_specs=placed,
        out_specs=(P("wlk", "pts"), P("wlk"), P("wlk")),
        check_vma=False,
    )
```

```python
import jax
import jax.numpy as jnp
from jax import lax
from jax.experimental import pallas as pl
from jax.experimental.pallas import tpu as pltpu
from jax.sharding import PartitionSpec as P


F32 = jnp.float32
BF16 = jnp.bfloat16
PLANES, COLS, CORES = 2, 4, 2
ZLO, YS = 2, 4
EXTRA = 8
OWN, LEFT, RIGHT, SIDE, PLANE, FAR, SIDE2, FAR2 = "olrspfgh"
SLOTS = {
    LEFT: ((0, 3), (0, 3)),
    RIGHT: ((0, 1), (0, 1)),
    SIDE: ((1, 3), (1, 1)),
    PLANE: ((1, 0), (1, 0)),
    FAR: ((0, 2), (0, 2)),
    SIDE2: ((1, 1), (1, 3)),
    FAR2: ((1, 2), (1, 2)),
}
AXES = ("pts", "wlk")


def whole():
    return pl.BlockSpec(memory_space=pltpu.VMEM)


def scalars():
    return pl.BlockSpec(memory_space=pltpu.SMEM)


def call(body, shapes, operands, mib, flops=0, **more):
    return pl.pallas_call(
        body,
        in_specs=[scalars()] + [whole()] * (len(operands) - 1),
        out_specs=jax.tree.map(lambda _: whole(), shapes),
        out_shape=shapes,
        cost_estimate=pl.CostEstimate(flops=flops, bytes_accessed=flops // 300, transcendentals=0),
        compiler_params=pltpu.CompilerParams(vmem_limit_bytes=mib << 20),
        **more,
    )(*operands)


def pts_id(a, x, c):
    return ((a & (PLANES - 1)) * COLS + (x & (COLS - 1))) * CORES + (c & (CORES - 1))


def from_device(block, source):
    route = []
    for a in range(PLANES):
        for x in range(COLS):
            for c in range(CORES):
                for z in range(ZLO):
                    for y in range(YS):
                        sa, sx, sc, sz, sy = source(a, x, c, z, y)
                        start = pts_id(sa, sx, sc) * ZLO * YS + (sz & 1) * YS + (sy & 3)
                        route.append((start, pts_id(a, x, c) * ZLO * YS + z * YS + y))
    return lax.ppermute(block, AXES, route)


def from_chip(block, da, dx, dc=0):
    return from_device(block, lambda a, x, c, z, y: (a + da, x + dx, c + dc, z, y))


def from_group(block, dz, dy):
    return from_device(block, lambda a, x, c, z, y: (a, x, c, z + dz, y + dy))


def from_column(block, slot):
    def source(a, x, c, z, y):
        return a, x + SLOTS[slot][(y ^ c) & 1][1], c, z, y

    return from_device(block, source)


def place(ids_ref):
    here = ids_ref[0]
    return here >> 3, (here >> 1) & 3, here & 1, ids_ref[1] & 3


def takes(slot, a, x, c, odd):
    low = jnp.where((x & 3) < COLS // 2, 1, 0)
    return {
        OWN: c,
        LEFT: 0,
        RIGHT: 1,
        SIDE: odd,
        PLANE: a,
        FAR: 1 - low,
        SIDE2: 1 - odd,
        FAR2: low,
    }[slot]


def chip_of(slot, a, x, odd):
    (a0, x0), (a1, x1) = SLOTS.get(slot, ((0, 0), (0, 0)))
    return a + jnp.where(odd == 1, a1, a0), x + jnp.where(odd == 1, x1, x0)


def split_columns(array, pieces, steps, mib):
    rows, cols = array.shape
    width = cols // pieces
    tile = rows // steps

    def body(x_ref, o_ref):
        @pl.loop(0, tile // 40)
        def _(part):
            cut = pl.ds(pl.multiple_of(part * 40, 8), 40)
            for b in range(pieces):
                o_ref[b, cut, :] = x_ref[cut, b * width : (b + 1) * width]

    return pl.pallas_call(
        body,
        grid=(steps,),
        in_specs=[pl.BlockSpec((tile, cols), lambda i: (i, 0))],
        out_specs=pl.BlockSpec((pieces, tile, width), lambda i: (0, i, 0)),
        out_shape=jax.ShapeDtypeStruct((pieces, rows, width), array.dtype),
        compiler_params=pltpu.CompilerParams(vmem_limit_bytes=mib << 20),
    )(array)


def pick(ids, takes_second, one, two):
    def body(ids_ref, one_ref, two_ref, o_ref):
        second = takes_second(*place(ids_ref))

        @pl.when(second == 0)
        def _():
            o_ref[...] = one_ref[...]

        @pl.when(second != 0)
        def _():
            o_ref[...] = two_ref[...]

    return call(body, jax.ShapeDtypeStruct(one.shape, one.dtype), [ids, one, two], 4)


def group_block(ids_ref, key):
    zlo, y = ids_ref[1] >> 2, ids_ref[1] & 3
    return ((zlo + key[0]) & (ZLO - 1)) * YS + ((y + key[1]) & (YS - 1))


def theta_part(ids, green_cut, blocks, so_far=None, occ_t=None):
    keys = list(blocks)
    n = len(keys)
    rows = green_cut.shape[1]
    pts = blocks[keys[0]].shape[1]
    flops = 2 * rows * pts * green_cut.shape[2] * n
    operands = [ids, green_cut, *blocks.values()]
    if so_far is not None:
        operands.append(so_far)

    if occ_t is None:

        def part(ids_ref, g_ref, *refs):
            cs, o_ref = refs[:n], refs[-1]
            at = [group_block(ids_ref, key) for key in keys]

            @pl.loop(0, 2)
            def _(half):
                cut = pl.ds(pl.multiple_of(half * (rows // 2), 8), rows // 2)
                total = sum(
                    jnp.dot(g_ref[at[j], cut, :], cs[j][...], preferred_element_type=F32)
                    for j in range(n)
                )
                o_ref[cut, :] = total if so_far is None else refs[n][cut, :] + total

        return call(part, jax.ShapeDtypeStruct((rows, pts), F32), operands, 8, flops)

    elec = occ_t.shape[0]

    def last(ids_ref, g_ref, *refs):
        cs = refs[:n]
        acc_ref, occ_ref, t0_ref, t1_ref, *pick_refs, dens_ref = refs[n:]
        at = [group_block(ids_ref, key) for key in keys]
        th_refs = (t0_ref, t1_ref)
        occ = occ_ref[...].astype(F32)
        dens = []
        for w in range(2):
            cut = pl.ds(w * elec, elec)
            t = acc_ref[cut, :] + sum(
                jnp.dot(g_ref[at[j], cut, :], cs[j][...], preferred_element_type=F32)
                for j in range(n)
            )
            t = t.astype(BF16)
            th_refs[w][0:elec, :] = t
            dens.append(jnp.sum(t.astype(F32) * occ, axis=0, keepdims=True))
        dens_ref[0:1, :] = dens[0]
        dens_ref[1:2, :] = dens[1]
        row = lax.broadcasted_iota(jnp.int32, (EXTRA, pts), 0)
        tail = jnp.where(row == 0, dens[0], jnp.where(row == 1, dens[1], 0.0)).astype(BF16)
        for w in range(2):
            th_refs[w][elec : elec + EXTRA, :] = tail
        a, x, c, y = place(ids_ref)
        odd = (y ^ c) & 1
        goes = (
            odd,
            1 - odd,
            takes(FAR, a, x + 2, c, odd),
            takes(OWN, a, x, 1 - c, odd),
        )
        for w, o_ref in zip(goes, pick_refs):

            @pl.when(w == 0)
            def _():
                o_ref[...] = t0_ref[...]

            @pl.when(w != 0)
            def _():
                o_ref[...] = t1_ref[...]

    slab = jax.ShapeDtypeStruct((elec + EXTRA, pts), BF16)
    shapes = [slab] * 6 + [jax.ShapeDtypeStruct((2, pts), F32)]
    return call(last, shapes, operands + [occ_t], 8, flops)


def exchange(jobs, ids, own, kernel_cut, acc=None, density=None):
    n = len(jobs)
    elec, pts = jobs[0][3][0].shape
    contract_last = (((1,), (1,)), ((), ()))
    occ_blocks = [block for job in jobs for block in job[3]]
    n_occ = len(occ_blocks)
    first = acc is None

    def body(ids_ref, k_ref, *refs):
        os, ts, refs = refs[:n_occ], refs[n_occ : n_occ + n], refs[n_occ + n :]
        a, x, c, y = place(ids_ref)
        if first:
            ex_ref, pot_ref, own_ref, flip_ref = refs
            ex_ref[...] = jnp.zeros_like(ex_ref)
            pot_ref[...] = jnp.zeros_like(pot_ref)
            for to, block in enumerate((ts[0], ts[1], os[0])):
                flip_ref[0:elec, 0:pts] = block[0:elec, :].astype(F32)
                own_ref[to] = flip_ref[...].T[0:pts, 0:elec].astype(BF16)
        elif density is None:
            own_ref, _, _, ex_ref, pot_ref = refs
        else:
            own_ref, _, _, dens_ref, ex_ref, pot_ref, pot_out, vals_out = refs
        for j, (slot, core, walker, blocks, _, weight, adds) in enumerate(jobs):
            odd = (y ^ c ^ core) & 1
            w = takes(slot, a, x, c, odd) if walker is None else walker
            k = k_ref[pts_id(*chip_of(slot, a, x, odd), c + core)]
            if len(blocks) > 1:
                occ = jnp.where(odd == 0, os[0][...], os[1][...])
            else:
                occ = os[j][...]
            near = jnp.dot(own_ref[w], occ, preferred_element_type=F32)
            far = jnp.dot(own_ref[2], ts[j][0:elec, :], preferred_element_type=F32)
            prod = k.astype(F32) * near * far
            ex_ref[w] += weight * jnp.sum(prod.reshape(pts // 8, 8, pts), axis=0)
            if adds:
                dens = ts[j][elec : elec + EXTRA, :]
                pot_ref[...] += lax.dot_general(
                    dens, k, contract_last, preferred_element_type=F32
                )
        if density is not None:
            pot = pot_ref[0:2, :]
            pot_out[...] = pot
            lane = lax.broadcasted_iota(jnp.int32, (8, 128), 1)
            vals = jnp.zeros((8, 128), F32)
            for w in range(2):
                coulomb = 0.5 * jnp.sum(dens_ref[w : w + 1, :] * pot[w : w + 1, :])
                vals = jnp.where(lane == w, coulomb, vals)
                vals = jnp.where(lane == 2 + w, -0.5 * jnp.sum(ex_ref[w]), vals)
            vals_out[...] = vals

    shapes = [jax.ShapeDtypeStruct((2, 8, pts), F32), jax.ShapeDtypeStruct((EXTRA, pts), F32)]
    operands = [ids, kernel_cut] + occ_blocks + [job[4] for job in jobs]
    scratch, alias = [], {}
    if first:
        shapes += [jax.ShapeDtypeStruct((3, pts, elec), BF16)]
        scratch = [pltpu.VMEM((-(-elec // 128) * 128, -(-pts // 128) * 128), F32)]
    else:
        operands += [own]
        alias = {len(operands): 0, len(operands) + 1: 1}
        operands += acc
    if density is not None:
        operands += [density]
        shapes += [jax.ShapeDtypeStruct((2, pts), F32), jax.ShapeDtypeStruct((8, 128), F32)]
    flops = 4 * pts * pts * elec * n
    return call(
        body, shapes, operands, 8, flops, scratch_shapes=scratch, input_output_aliases=alias
    )


def everyone_total(v):
    v = v + from_chip(v, 0, 0, 1)
    r1, r2, r3 = (from_chip(v, 0, dx) for dx in (1, 2, 3))
    v = (v + r2) + (r1 + r3)
    return v + from_chip(v, 1, 0)


def local(green_half, collocation, occupied, kernel):
    walkers, elec, orb = green_half.shape
    ids = jnp.stack([lax.axis_index(axis) for axis in AXES]).astype(jnp.int32)
    occ_t = occupied.T

    coll = {(0, 0): collocation}
    coll[1, 0] = from_group(collocation, 1, 0)
    for dy in (2, 1, 3):
        coll[0, dy] = from_group(collocation, 0, dy)
    for dy in (1, 3):
        coll[1, dy] = from_group(coll[1, 0], 0, dy)
    coll[1, 2] = from_group(coll[0, 2], 1, 0)
    occ_left = from_column(occ_t, LEFT)
    occ_right = from_column(occ_t, RIGHT)
    occ_plane = from_chip(occ_t, 1, 0)
    occ_side = from_column(occ_plane, SIDE)
    occ_pick = pick(ids, lambda a, x, c, y: (y ^ c) & 1, occ_t, occ_plane)
    occ_far = from_column(occ_pick, FAR)

    def from_y(block):
        return from_device(block, lambda a, x, c, z, y: (a, x, c, z, y ^ 1))

    occ_side2 = from_y(occ_side)
    occ_far2 = from_y(occ_far)
    occ = {OWN: [occ_t], LEFT: [occ_left], RIGHT: [occ_right], FAR: [occ_far, occ_far2]}
    occ |= {SIDE: [occ_side], PLANE: [occ_plane], SIDE2: [occ_side2]}

    green = green_half.reshape(walkers * elec, orb)
    green_cut = split_columns(green, ZLO * YS, 4, 8)
    kernel_cut = split_columns(kernel, PLANES * COLS * CORES, 5, 12)

    def some(keys):
        return {k: coll[k] for k in keys}

    so_far = theta_part(ids, green_cut, some([(0, 0), (1, 0), (0, 2)]))
    middle = some([(0, 1), (0, 3), (1, 1), (1, 3)])
    so_far = theta_part(ids, green_cut, middle, so_far)
    t0, t1, t_first, t_second, t_far, t_sib, density = theta_part(
        ids, green_cut, some([(1, 2)]), so_far, occ_t
    )
    first = from_chip(t_first, 1, 0)
    second = from_chip(t_second, 1, 0)
    plane = pick(ids, lambda a, x, c, y: a ^ (y ^ c) & 1, first, second)
    far2 = pick(ids, lambda a, x, c, y: x >> 1 ^ (y ^ c) & 1, first, second)
    sends = {LEFT: t0, RIGHT: t1, FAR: t_far, SIDE: first, SIDE2: second, FAR2: far2}
    theta = {slot: from_column(sends[slot], slot) for slot in sends}
    theta |= {OWN: t_sib, PLANE: plane}
    theta_sib = {slot: from_chip(theta[slot], 0, 0, 1) for slot in theta}
    occ_sib = {slot: [from_chip(occ[slot][0], 0, 0, 1)] for slot in occ}
    occ_sib[FAR] += [from_chip(occ_far2, 0, 0, 1)]
    for known in (occ, occ_sib):
        known[FAR2] = known[FAR][::-1]

    own_jobs = [(OWN, 0, w, [occ_t], t, 1.0, w == 0) for w, t in enumerate((t0, t1))]
    *acc, own = exchange(own_jobs, ids, None, kernel_cut)

    for slot in (OWN, *SLOTS):
        if slot != OWN:
            same = (slot, 0, None, occ[slot], theta[slot], 2.0, True)
            acc = exchange([same], ids, own, kernel_cut, acc)
        sib = (slot, 1, None, occ_sib[slot], theta_sib[slot], 2.0, True)
        ending = density if slot == FAR2 else None
        acc = exchange([sib], ids, own, kernel_cut, acc, ending)
    _, _, potential, energies = acc
    energies = everyone_total(energies)
    return potential, energies[0, :walkers], energies[0, walkers : 2 * walkers]


def solution(mesh):
    split = P("wlk", "pts")
    placed = (P("wlk", None, None), split, P("pts", None), P("pts", None))

    return jax.shard_map(
        local,
        mesh=mesh,
        in_specs=placed,
        out_specs=(split, P("wlk"), P("wlk")),
        check_vma=False,
    )
```

```python
import jax
import jax.numpy as jnp
from jax import lax
from jax.experimental import pallas as pl
from jax.experimental.pallas import tpu as pltpu
from jax.sharding import PartitionSpec as P


F32 = jnp.float32
BF16 = jnp.bfloat16
PLANES, COLS, CORES = 2, 4, 2
ZLO, YS = 2, 4
EXTRA = 8
OWN, LEFT, RIGHT, SIDE, PLANE, FAR, SIDE2, FAR2 = "olrspfgh"
SLOTS = {
    LEFT: ((0, 3), (0, 3)),
    RIGHT: ((0, 1), (0, 1)),
    SIDE: ((1, 3), (1, 1)),
    PLANE: ((1, 0), (1, 0)),
    FAR: ((0, 2), (0, 2)),
    SIDE2: ((1, 1), (1, 3)),
    FAR2: ((1, 2), (1, 2)),
}
AXES = ("pts", "wlk")


def whole():
    return pl.BlockSpec(memory_space=pltpu.VMEM)


def call(body, shapes, operands, mib, flops=0, **more):
    return pl.pallas_call(
        body,
        in_specs=[whole()] * len(operands),
        out_specs=jax.tree.map(lambda _: whole(), shapes),
        out_shape=shapes,
        cost_estimate=pl.CostEstimate(flops=flops, bytes_accessed=flops // 300, transcendentals=0),
        compiler_params=pltpu.CompilerParams(vmem_limit_bytes=mib << 20),
        **more,
    )(*operands)


def pts_id(a, x, c):
    return ((a & (PLANES - 1)) * COLS + (x & (COLS - 1))) * CORES + (c & (CORES - 1))


def from_device(block, source):
    route = []
    for a in range(PLANES):
        for x in range(COLS):
            for c in range(CORES):
                for z in range(ZLO):
                    for y in range(YS):
                        sa, sx, sc, sz, sy = source(a, x, c, z, y)
                        start = pts_id(sa, sx, sc) * ZLO * YS + (sz & 1) * YS + (sy & 3)
                        route.append((start, pts_id(a, x, c) * ZLO * YS + z * YS + y))
    return lax.ppermute(block, AXES, route)


def from_chip(block, da, dx, dc=0):
    return from_device(block, lambda a, x, c, z, y: (a + da, x + dx, c + dc, z, y))


def from_group(block, dz, dy):
    return from_device(block, lambda a, x, c, z, y: (a, x, c, z + dz, y + dy))


def from_column(block, slot):
    def source(a, x, c, z, y):
        return a, x + SLOTS[slot][(y ^ c) & 1][1], c, z, y

    return from_device(block, source)


def onward(block, step, columns):
    route = []
    for a in range(PLANES):
        for x in columns:
            for c in range(CORES):
                route.append((pts_id(a, x - step, c), pts_id(a, x, c)))
    return lax.ppermute(block, AXES[0], route)


def place():
    here = lax.axis_index(AXES[0])
    return here >> 3, (here >> 1) & 3, here & 1, lax.axis_index(AXES[1]) & 3


def takes(slot, a, x, c, odd):
    low = jnp.where((x & 3) < COLS // 2, 1, 0)
    return {
        OWN: c,
        LEFT: 0,
        RIGHT: 1,
        SIDE: odd,
        PLANE: a,
        FAR: 1 - low,
        SIDE2: 1 - odd,
        FAR2: low,
    }[slot]


def chip_of(slot, a, x, odd):
    (a0, x0), (a1, x1) = SLOTS.get(slot, ((0, 0), (0, 0)))
    return a + jnp.where(odd == 1, a1, a0), x + jnp.where(odd == 1, x1, x0)


def split_columns(array, pieces, steps, mib):
    rows, cols = array.shape
    width = cols // pieces
    tile = rows // steps

    def body(x_ref, o_ref):
        @pl.loop(0, tile // 40)
        def _(part):
            cut = pl.ds(pl.multiple_of(part * 40, 8), 40)
            for b in range(pieces):
                o_ref[b, cut, :] = x_ref[cut, b * width : (b + 1) * width]

    return pl.pallas_call(
        body,
        grid=(steps,),
        in_specs=[pl.BlockSpec((tile, cols), lambda i: (i, 0))],
        out_specs=pl.BlockSpec((pieces, tile, width), lambda i: (0, i, 0)),
        out_shape=jax.ShapeDtypeStruct((pieces, rows, width), array.dtype),
        compiler_params=pltpu.CompilerParams(vmem_limit_bytes=mib << 20),
    )(array)


def pick(takes_second, one, two):
    def body(one_ref, two_ref, o_ref):
        second = takes_second(*place())

        @pl.when(second == 0)
        def _():
            o_ref[...] = one_ref[...]

        @pl.when(second != 0)
        def _():
            o_ref[...] = two_ref[...]

    return call(body, jax.ShapeDtypeStruct(one.shape, one.dtype), [one, two], 4)


def group_block(key):
    group = lax.axis_index(AXES[1])
    zlo, y = group >> 2, group & 3
    return ((zlo + key[0]) & (ZLO - 1)) * YS + ((y + key[1]) & (YS - 1))


def theta_part(green_cut, blocks, so_far=None, occ_t=None):
    keys = list(blocks)
    n = len(keys)
    rows = green_cut.shape[1]
    pts = blocks[keys[0]].shape[1]
    flops = 2 * rows * pts * green_cut.shape[2] * n
    operands = [green_cut, *blocks.values()]
    if so_far is not None:
        operands.append(so_far)

    if occ_t is None:

        def part(g_ref, *refs):
            cs, o_ref = refs[:n], refs[-1]
            at = [group_block(key) for key in keys]

            @pl.loop(0, 2)
            def _(half):
                cut = pl.ds(pl.multiple_of(half * (rows // 2), 8), rows // 2)
                total = sum(
                    jnp.dot(g_ref[at[j], cut, :], cs[j][...], preferred_element_type=F32)
                    for j in range(n)
                )
                o_ref[cut, :] = total if so_far is None else refs[n][cut, :] + total

        return call(part, jax.ShapeDtypeStruct((rows, pts), F32), operands, 8, flops)

    elec = occ_t.shape[0]

    def last(g_ref, *refs):
        cs = refs[:n]
        acc_ref, occ_ref, t0_ref, t1_ref, *pick_refs, dens_ref = refs[n:]
        at = [group_block(key) for key in keys]
        th_refs = (t0_ref, t1_ref)
        occ = occ_ref[...].astype(F32)
        dens = []
        for w in range(2):
            cut = pl.ds(w * elec, elec)
            t = acc_ref[cut, :] + sum(
                jnp.dot(g_ref[at[j], cut, :], cs[j][...], preferred_element_type=F32)
                for j in range(n)
            )
            t = t.astype(BF16)
            th_refs[w][0:elec, :] = t
            dens.append(jnp.sum(t.astype(F32) * occ, axis=0, keepdims=True))
        dens_ref[0:1, :] = dens[0]
        dens_ref[1:2, :] = dens[1]
        row = lax.broadcasted_iota(jnp.int32, (EXTRA, pts), 0)
        tail = jnp.where(row == 0, dens[0], jnp.where(row == 1, dens[1], 0.0)).astype(BF16)
        for w in range(2):
            th_refs[w][elec : elec + EXTRA, :] = tail
        a, x, c, y = place()
        odd = (y ^ c) & 1
        goes = (
            odd,
            1 - odd,
            takes(OWN, a, x, 1 - c, odd),
        )
        for w, o_ref in zip(goes, pick_refs):

            @pl.when(w == 0)
            def _():
                o_ref[...] = t0_ref[...]

            @pl.when(w != 0)
            def _():
                o_ref[...] = t1_ref[...]

    slab = jax.ShapeDtypeStruct((elec + EXTRA, pts), BF16)
    shapes = [slab] * 5 + [jax.ShapeDtypeStruct((2, pts), F32)]
    return call(last, shapes, operands + [occ_t], 8, flops)


def exchange(jobs, own, kernel_cut, acc=None, density=None):
    n = len(jobs)
    elec, pts = jobs[0][3][0].shape
    contract_last = (((1,), (1,)), ((), ()))
    occ_blocks = [block for job in jobs for block in job[3]]
    n_occ = len(occ_blocks)
    first = acc is None

    def body(k_ref, *refs):
        os, ts, refs = refs[:n_occ], refs[n_occ : n_occ + n], refs[n_occ + n :]
        a, x, c, y = place()
        if first:
            ex_ref, pot_ref, own_ref, flip_ref = refs
            ex_ref[...] = jnp.zeros_like(ex_ref)
            pot_ref[...] = jnp.zeros_like(pot_ref)
            for to, block in enumerate((ts[0], ts[1], os[0])):
                flip_ref[0:elec, 0:pts] = block[0:elec, :].astype(F32)
                own_ref[to] = flip_ref[...].T[0:pts, 0:elec].astype(BF16)
        elif density is None:
            own_ref, _, _, ex_ref, pot_ref = refs
        else:
            own_ref, _, _, dens_ref, ex_ref, pot_ref, pot_out, vals_out = refs
        for j, (slot, core, walker, blocks, _, weight, adds) in enumerate(jobs):
            odd = (y ^ c ^ core) & 1
            w = takes(slot, a, x, c, odd) if walker is None else walker
            k = k_ref[pts_id(*chip_of(slot, a, x, odd), c + core)]
            if len(blocks) > 1:
                occ = jnp.where(odd == 0, os[0][...], os[1][...])
            else:
                occ = os[j][...]
            near = jnp.dot(own_ref[w], occ, preferred_element_type=F32)
            far = jnp.dot(own_ref[2], ts[j][0:elec, :], preferred_element_type=F32)
            prod = k.astype(F32) * near * far
            ex_ref[w] += weight * jnp.sum(prod.reshape(pts // 8, 8, pts), axis=0)
            if adds:
                dens = ts[j][elec : elec + EXTRA, :]
                pot_ref[...] += lax.dot_general(
                    dens, k, contract_last, preferred_element_type=F32
                )
        if density is not None:
            pot = pot_ref[0:2, :]
            pot_out[...] = pot
            lane = lax.broadcasted_iota(jnp.int32, (8, 128), 1)
            vals = jnp.zeros((8, 128), F32)
            for w in range(2):
                coulomb = 0.5 * jnp.sum(dens_ref[w : w + 1, :] * pot[w : w + 1, :])
                vals = jnp.where(lane == w, coulomb, vals)
                vals = jnp.where(lane == 2 + w, -0.5 * jnp.sum(ex_ref[w]), vals)
            vals_out[...] = vals

    shapes = [jax.ShapeDtypeStruct((2, 8, pts), F32), jax.ShapeDtypeStruct((EXTRA, pts), F32)]
    operands = [kernel_cut] + occ_blocks + [job[4] for job in jobs]
    scratch, alias = [], {}
    if first:
        shapes += [jax.ShapeDtypeStruct((3, pts, elec), BF16)]
        scratch = [pltpu.VMEM((-(-elec // 128) * 128, -(-pts // 128) * 128), F32)]
    else:
        operands += [own]
        alias = {len(operands): 0, len(operands) + 1: 1}
        operands += acc
    if density is not None:
        operands += [density]
        shapes += [jax.ShapeDtypeStruct((2, pts), F32), jax.ShapeDtypeStruct((8, 128), F32)]
    flops = 4 * pts * pts * elec * n
    return call(
        body, shapes, operands, 8, flops, scratch_shapes=scratch, input_output_aliases=alias
    )


def everyone_total(v):
    v = v + from_chip(v, 0, 0, 1)
    r1, r2, r3 = (from_chip(v, 0, dx) for dx in (1, 2, 3))
    v = (v + r2) + (r1 + r3)
    return v + from_chip(v, 1, 0)


def local(green_half, collocation, occupied, kernel):
    walkers, elec, orb = green_half.shape
    occ_t = occupied.T

    coll = {(0, 0): collocation}
    coll[1, 0] = from_group(collocation, 1, 0)
    for dy in (2, 1, 3):
        coll[0, dy] = from_group(collocation, 0, dy)
    for dy in (1, 3):
        coll[1, dy] = from_group(coll[1, 0], 0, dy)
    coll[1, 2] = from_group(coll[0, 2], 1, 0)
    occ_left = from_column(occ_t, LEFT)
    occ_right = from_column(occ_t, RIGHT)
    occ_plane = from_chip(occ_t, 1, 0)
    occ_side = from_column(occ_plane, SIDE)
    occ_pick = pick(lambda a, x, c, y: (y ^ c) & 1, occ_t, occ_plane)
    occ_far = from_column(occ_pick, FAR)

    def from_y(block):
        return from_device(block, lambda a, x, c, z, y: (a, x, c, z, y ^ 1))

    occ_side2 = from_y(occ_side)
    occ_far2 = from_y(occ_far)
    occ = {OWN: [occ_t], LEFT: [occ_left], RIGHT: [occ_right], FAR: [occ_far, occ_far2]}
    occ |= {SIDE: [occ_side], PLANE: [occ_plane], SIDE2: [occ_side2]}

    green = green_half.reshape(walkers * elec, orb)
    green_cut = split_columns(green, ZLO * YS, 4, 8)
    kernel_cut = split_columns(kernel, PLANES * COLS * CORES, 5, 12)

    def some(keys):
        return {k: coll[k] for k in keys}

    so_far = theta_part(green_cut, some([(0, 0), (1, 0), (0, 2)]))
    so_far = theta_part(green_cut, some([(0, 1), (0, 3)]), so_far)
    so_far = theta_part(green_cut, some([(1, 1), (1, 3)]), so_far)
    t0, t1, t_first, t_second, t_sib, density = theta_part(green_cut, some([(1, 2)]), so_far, occ_t)
    first = from_chip(t_first, 1, 0)
    second = from_chip(t_second, 1, 0)
    theta = {OWN: t_sib}
    sends = {LEFT: t0, RIGHT: t1, SIDE: first, SIDE2: second}
    for slot, block in sends.items():
        theta[slot] = from_column(block, slot)
    theta[PLANE] = pick(lambda a, x, c, y: a ^ (y ^ c) & 1, first, second)

    def right_half(a, x, c, y):
        return x >> 1

    right = onward(theta[LEFT], 1, (0, 1))
    left = onward(theta[RIGHT], -1, (2, 3))
    theta[FAR] = pick(right_half, right, left)
    side, side2 = theta[SIDE], theta[SIDE2]
    walker0 = pick(lambda a, x, c, y: (y ^ c) & 1, side, side2)
    walker1 = pick(lambda a, x, c, y: (y ^ c) & 1, side2, side)
    right = onward(walker0, 1, (2, 3))
    left = onward(walker1, -1, (0, 1))
    theta[FAR2] = pick(right_half, left, right)
    theta_sib = {slot: from_chip(theta[slot], 0, 0, 1) for slot in theta}
    occ_sib = {slot: [from_chip(occ[slot][0], 0, 0, 1)] for slot in occ}
    occ_sib[FAR] += [from_chip(occ_far2, 0, 0, 1)]
    for known in (occ, occ_sib):
        known[FAR2] = known[FAR][::-1]

    own_jobs = [(OWN, 0, w, [occ_t], t, 1.0, w == 0) for w, t in enumerate((t0, t1))]
    *acc, own = exchange(own_jobs, None, kernel_cut)

    for slot in (OWN, *SLOTS):
        if slot != OWN:
            same = (slot, 0, None, occ[slot], theta[slot], 2.0, True)
            acc = exchange([same], own, kernel_cut, acc)
        sib = (slot, 1, None, occ_sib[slot], theta_sib[slot], 2.0, True)
        ending = density if slot == FAR2 else None
        acc = exchange([sib], own, kernel_cut, acc, ending)
    _, _, potential, energies = acc
    energies = everyone_total(energies)
    return potential, energies[0, :walkers], energies[0, walkers : 2 * walkers]


def solution(mesh):
    split = P("wlk", "pts")
    placed = (P("wlk", None, None), split, P("pts", None), P("pts", None))

    return jax.shard_map(
        local,
        mesh=mesh,
        in_specs=placed,
        out_specs=(split, P("wlk"), P("wlk")),
        check_vma=False,
    )
```

```python
import jax
import jax.numpy as jnp
from jax import lax
from jax.experimental import pallas as pl
from jax.experimental.pallas import tpu as pltpu
from jax.sharding import PartitionSpec as P


F32 = jnp.float32
BF16 = jnp.bfloat16
PLANES, COLS, CORES = 2, 4, 2
ZLO, YS = 2, 4
EXTRA = 8
OWN, LEFT, RIGHT, SIDE, PLANE, FAR, SIDE2, FAR2 = "olrspfgh"
SLOTS = {
    LEFT: ((0, 3), (0, 3)),
    RIGHT: ((0, 1), (0, 1)),
    SIDE: ((1, 3), (1, 1)),
    PLANE: ((1, 0), (1, 0)),
    FAR: ((0, 2), (0, 2)),
    SIDE2: ((1, 1), (1, 3)),
    FAR2: ((1, 2), (1, 2)),
}
AXES = ("pts", "wlk")


def whole():
    return pl.BlockSpec(memory_space=pltpu.VMEM)


def call(body, shapes, operands, mib, flops=0, **more):
    return pl.pallas_call(
        body,
        in_specs=[whole()] * len(operands),
        out_specs=jax.tree.map(lambda _: whole(), shapes),
        out_shape=shapes,
        cost_estimate=pl.CostEstimate(flops=flops, bytes_accessed=flops // 300, transcendentals=0),
        compiler_params=pltpu.CompilerParams(vmem_limit_bytes=mib << 20),
        **more,
    )(*operands)


def pts_id(a, x, c):
    return ((a & (PLANES - 1)) * COLS + (x & (COLS - 1))) * CORES + (c & (CORES - 1))


def from_device(block, source):
    route = []
    for a in range(PLANES):
        for x in range(COLS):
            for c in range(CORES):
                for z in range(ZLO):
                    for y in range(YS):
                        sa, sx, sc, sz, sy = source(a, x, c, z, y)
                        start = pts_id(sa, sx, sc) * ZLO * YS + (sz & 1) * YS + (sy & 3)
                        route.append((start, pts_id(a, x, c) * ZLO * YS + z * YS + y))
    return lax.ppermute(block, AXES, route)


def from_chip(block, da, dx, dc=0):
    return from_device(block, lambda a, x, c, z, y: (a + da, x + dx, c + dc, z, y))


def from_group(block, dz, dy):
    return from_device(block, lambda a, x, c, z, y: (a, x, c, z + dz, y + dy))


def from_column(block, slot):
    def source(a, x, c, z, y):
        return a, x + SLOTS[slot][(y ^ c) & 1][1], c, z, y

    return from_device(block, source)


def onward(block, step, columns):
    route = []
    for a in range(PLANES):
        for x in columns:
            for c in range(CORES):
                route.append((pts_id(a, x - step, c), pts_id(a, x, c)))
    return lax.ppermute(block, AXES[0], route)


def onward_by_parity(block, rightward):
    route = []
    for a in range(PLANES):
        for x in range(COLS):
            for c in range(CORES):
                for z in range(ZLO):
                    for y in range(YS):
                        step = 1 if (y ^ c) & 1 == rightward else -1
                        if (x >= COLS // 2) == (step == 1):
                            at = z * YS + y
                            start = pts_id(a, x - step, c) * ZLO * YS + at
                            route.append((start, pts_id(a, x, c) * ZLO * YS + at))
    return lax.ppermute(block, AXES, route)


def place():
    here = lax.axis_index(AXES[0])
    return here >> 3, (here >> 1) & 3, here & 1, lax.axis_index(AXES[1]) & 3


def takes(slot, a, x, c, odd):
    low = jnp.where((x & 3) < COLS // 2, 1, 0)
    return {
        OWN: c,
        LEFT: 0,
        RIGHT: 1,
        SIDE: odd,
        PLANE: a,
        FAR: 1 - low,
        SIDE2: 1 - odd,
        FAR2: low,
    }[slot]


def chip_of(slot, a, x, odd):
    (a0, x0), (a1, x1) = SLOTS.get(slot, ((0, 0), (0, 0)))
    return a + jnp.where(odd == 1, a1, a0), x + jnp.where(odd == 1, x1, x0)


def split_columns(array, pieces, steps, mib):
    rows, cols = array.shape
    width = cols // pieces
    tile = rows // steps

    def body(x_ref, o_ref):
        @pl.loop(0, tile // 40)
        def _(part):
            cut = pl.ds(pl.multiple_of(part * 40, 8), 40)
            for b in range(pieces):
                o_ref[b, cut, :] = x_ref[cut, b * width : (b + 1) * width]

    return pl.pallas_call(
        body,
        grid=(steps,),
        in_specs=[pl.BlockSpec((tile, cols), lambda i: (i, 0))],
        out_specs=pl.BlockSpec((pieces, tile, width), lambda i: (0, i, 0)),
        out_shape=jax.ShapeDtypeStruct((pieces, rows, width), array.dtype),
        compiler_params=pltpu.CompilerParams(vmem_limit_bytes=mib << 20),
    )(array)


def pick(takes_second, one, two):
    def body(one_ref, two_ref, o_ref):
        second = takes_second(*place())

        @pl.when(second == 0)
        def _():
            o_ref[...] = one_ref[...]

        @pl.when(second != 0)
        def _():
            o_ref[...] = two_ref[...]

    return call(body, jax.ShapeDtypeStruct(one.shape, one.dtype), [one, two], 4)


def group_block(key):
    group = lax.axis_index(AXES[1])
    zlo, y = group >> 2, group & 3
    return ((zlo + key[0]) & (ZLO - 1)) * YS + ((y + key[1]) & (YS - 1))


def theta_part(green_cut, blocks, so_far=None, occ_t=None):
    keys = list(blocks)
    n = len(keys)
    rows = green_cut.shape[1]
    pts = blocks[keys[0]].shape[1]
    flops = 2 * rows * pts * green_cut.shape[2] * n
    operands = [green_cut, *blocks.values()]
    if so_far is not None:
        operands.append(so_far)

    if occ_t is None:

        def part(g_ref, *refs):
            cs, o_ref = refs[:n], refs[-1]
            at = [group_block(key) for key in keys]

            @pl.loop(0, 2)
            def _(half):
                cut = pl.ds(pl.multiple_of(half * (rows // 2), 8), rows // 2)
                total = sum(
                    jnp.dot(g_ref[at[j], cut, :], cs[j][...], preferred_element_type=F32)
                    for j in range(n)
                )
                o_ref[cut, :] = total if so_far is None else refs[n][cut, :] + total

        return call(part, jax.ShapeDtypeStruct((rows, pts), F32), operands, 8, flops)

    elec = occ_t.shape[0]

    def last(g_ref, *refs):
        cs = refs[:n]
        acc_ref, occ_ref, t0_ref, t1_ref, *pick_refs, dens_ref = refs[n:]
        at = [group_block(key) for key in keys]
        th_refs = (t0_ref, t1_ref)
        occ = occ_ref[...].astype(F32)
        dens = []
        for w in range(2):
            cut = pl.ds(w * elec, elec)
            t = acc_ref[cut, :] + sum(
                jnp.dot(g_ref[at[j], cut, :], cs[j][...], preferred_element_type=F32)
                for j in range(n)
            )
            t = t.astype(BF16)
            th_refs[w][0:elec, :] = t
            dens.append(jnp.sum(t.astype(F32) * occ, axis=0, keepdims=True))
        dens_ref[0:1, :] = dens[0]
        dens_ref[1:2, :] = dens[1]
        row = lax.broadcasted_iota(jnp.int32, (EXTRA, pts), 0)
        tail = jnp.where(row == 0, dens[0], jnp.where(row == 1, dens[1], 0.0)).astype(BF16)
        for w in range(2):
            th_refs[w][elec : elec + EXTRA, :] = tail
        a, x, c, y = place()
        odd = (y ^ c) & 1
        goes = (
            odd,
            1 - odd,
            takes(OWN, a, x, 1 - c, odd),
        )
        for w, o_ref in zip(goes, pick_refs):

            @pl.when(w == 0)
            def _():
                o_ref[...] = t0_ref[...]

            @pl.when(w != 0)
            def _():
                o_ref[...] = t1_ref[...]

    slab = jax.ShapeDtypeStruct((elec + EXTRA, pts), BF16)
    shapes = [slab] * 5 + [jax.ShapeDtypeStruct((2, pts), F32)]
    return call(last, shapes, operands + [occ_t], 8, flops)


def exchange(jobs, own, kernel_cut, acc=None, density=None):
    n = len(jobs)
    elec, pts = jobs[0][3][0].shape
    contract_last = (((1,), (1,)), ((), ()))
    occ_blocks = [block for job in jobs for block in job[3]]
    n_occ = len(occ_blocks)
    first = acc is None

    def body(k_ref, *refs):
        os, ts, refs = refs[:n_occ], refs[n_occ : n_occ + n], refs[n_occ + n :]
        a, x, c, y = place()
        if first:
            ex_ref, pot_ref, own_ref, flip_ref = refs
            ex_ref[...] = jnp.zeros_like(ex_ref)
            pot_ref[...] = jnp.zeros_like(pot_ref)
            for to, block in enumerate((ts[0], ts[1], os[0])):
                flip_ref[0:elec, 0:pts] = block[0:elec, :].astype(F32)
                own_ref[to] = flip_ref[...].T[0:pts, 0:elec].astype(BF16)
        elif density is None:
            own_ref, _, _, ex_ref, pot_ref = refs
        else:
            own_ref, _, _, dens_ref, ex_ref, pot_ref, pot_out, vals_out = refs
        for j, (slot, core, walker, blocks, _, weight, adds) in enumerate(jobs):
            odd = (y ^ c ^ core) & 1
            w = takes(slot, a, x, c, odd) if walker is None else walker
            k = k_ref[pts_id(*chip_of(slot, a, x, odd), c + core)]
            if len(blocks) > 1:
                occ = jnp.where(odd == 0, os[0][...], os[1][...])
            else:
                occ = os[j][...]
            near = jnp.dot(own_ref[w], occ, preferred_element_type=F32)
            far = jnp.dot(own_ref[2], ts[j][0:elec, :], preferred_element_type=F32)
            prod = k.astype(F32) * near * far
            ex_ref[w] += weight * jnp.sum(prod.reshape(pts // 8, 8, pts), axis=0)
            if adds:
                dens = ts[j][elec : elec + EXTRA, :]
                pot_ref[...] += lax.dot_general(
                    dens, k, contract_last, preferred_element_type=F32
                )
        if density is not None:
            pot = pot_ref[0:2, :]
            pot_out[...] = pot
            lane = lax.broadcasted_iota(jnp.int32, (8, 128), 1)
            vals = jnp.zeros((8, 128), F32)
            for w in range(2):
                coulomb = 0.5 * jnp.sum(dens_ref[w : w + 1, :] * pot[w : w + 1, :])
                vals = jnp.where(lane == w, coulomb, vals)
                vals = jnp.where(lane == 2 + w, -0.5 * jnp.sum(ex_ref[w]), vals)
            vals_out[...] = vals

    shapes = [jax.ShapeDtypeStruct((2, 8, pts), F32), jax.ShapeDtypeStruct((EXTRA, pts), F32)]
    operands = [kernel_cut] + occ_blocks + [job[4] for job in jobs]
    scratch, alias = [], {}
    if first:
        shapes += [jax.ShapeDtypeStruct((3, pts, elec), BF16)]
        scratch = [pltpu.VMEM((-(-elec // 128) * 128, -(-pts // 128) * 128), F32)]
    else:
        operands += [own]
        alias = {len(operands): 0, len(operands) + 1: 1}
        operands += acc
    if density is not None:
        operands += [density]
        shapes += [jax.ShapeDtypeStruct((2, pts), F32), jax.ShapeDtypeStruct((8, 128), F32)]
    flops = 4 * pts * pts * elec * n
    return call(
        body, shapes, operands, 8, flops, scratch_shapes=scratch, input_output_aliases=alias
    )


def everyone_total(v):
    v = v + from_chip(v, 0, 0, 1)
    r1, r2, r3 = (from_chip(v, 0, dx) for dx in (1, 2, 3))
    v = (v + r2) + (r1 + r3)
    return v + from_chip(v, 1, 0)


def local(green_half, collocation, occupied, kernel):
    walkers, elec, orb = green_half.shape
    occ_t = occupied.T

    coll = {(0, 0): collocation}
    coll[1, 0] = from_group(collocation, 1, 0)
    for dy in (2, 1, 3):
        coll[0, dy] = from_group(collocation, 0, dy)
    for dy in (1, 3):
        coll[1, dy] = from_group(coll[1, 0], 0, dy)
    coll[1, 2] = from_group(coll[0, 2], 1, 0)
    occ_left = from_column(occ_t, LEFT)
    occ_right = from_column(occ_t, RIGHT)
    occ_plane = from_chip(occ_t, 1, 0)
    occ_side = from_column(occ_plane, SIDE)
    occ_pick = pick(lambda a, x, c, y: (y ^ c) & 1, occ_t, occ_plane)
    occ_far = from_column(occ_pick, FAR)

    def from_y(block):
        return from_device(block, lambda a, x, c, z, y: (a, x, c, z, y ^ 1))

    occ_side2 = from_y(occ_side)
    occ_far2 = from_y(occ_far)
    occ = {OWN: [occ_t], LEFT: [occ_left], RIGHT: [occ_right], FAR: [occ_far, occ_far2]}
    occ |= {SIDE: [occ_side], PLANE: [occ_plane], SIDE2: [occ_side2]}

    green = green_half.reshape(walkers * elec, orb)
    green_cut = split_columns(green, ZLO * YS, 4, 8)
    kernel_cut = split_columns(kernel, PLANES * COLS * CORES, 5, 12)

    def some(keys):
        return {k: coll[k] for k in keys}

    so_far = theta_part(green_cut, some([(0, 0), (1, 0), (0, 2)]))
    so_far = theta_part(green_cut, some([(0, 1), (0, 3)]), so_far)
    so_far = theta_part(green_cut, some([(1, 1), (1, 3)]), so_far)
    t0, t1, t_first, t_second, t_sib, density = theta_part(green_cut, some([(1, 2)]), so_far, occ_t)
    first = from_chip(t_first, 1, 0)
    second = from_chip(t_second, 1, 0)
    theta = {OWN: t_sib}
    sends = {LEFT: t0, RIGHT: t1, SIDE: first, SIDE2: second}
    for slot, block in sends.items():
        theta[slot] = from_column(block, slot)
    theta[PLANE] = pick(lambda a, x, c, y: a ^ (y ^ c) & 1, first, second)

    def right_half(a, x, c, y):
        return x >> 1

    right = onward(theta[LEFT], 1, (0, 1))
    left = onward(theta[RIGHT], -1, (2, 3))
    theta[FAR] = pick(right_half, right, left)
    one = onward_by_parity(theta[SIDE], 0)
    two = onward_by_parity(theta[SIDE2], 1)
    theta[FAR2] = pick(lambda a, x, c, y: 1 ^ x >> 1 ^ (y ^ c) & 1, one, two)
    theta_sib = {slot: from_chip(theta[slot], 0, 0, 1) for slot in theta}
    occ_sib = {slot: [from_chip(occ[slot][0], 0, 0, 1)] for slot in occ}
    occ_sib[FAR] += [from_chip(occ_far2, 0, 0, 1)]
    for known in (occ, occ_sib):
        known[FAR2] = known[FAR][::-1]

    own_jobs = [(OWN, 0, w, [occ_t], t, 1.0, w == 0) for w, t in enumerate((t0, t1))]
    *acc, own = exchange(own_jobs, None, kernel_cut)

    for slot in (OWN, *SLOTS):
        if slot != OWN:
            same = (slot, 0, None, occ[slot], theta[slot], 2.0, True)
            acc = exchange([same], own, kernel_cut, acc)
        sib = (slot, 1, None, occ_sib[slot], theta_sib[slot], 2.0, True)
        ending = density if slot == FAR2 else None
        acc = exchange([sib], own, kernel_cut, acc, ending)
    _, _, potential, energies = acc
    energies = everyone_total(energies)
    return potential, energies[0, :walkers], energies[0, walkers : 2 * walkers]


def solution(mesh):
    split = P("wlk", "pts")
    placed = (P("wlk", None, None), split, P("pts", None), P("pts", None))

    return jax.shard_map(
        local,
        mesh=mesh,
        in_specs=placed,
        out_specs=(split, P("wlk"), P("wlk")),
        check_vma=False,
    )
```
